128 devices in a mesh: batch: 4 (over z), seq: 16 (over y, x_lo, core), head: 2 (over x_hi).
Axes of the slice: x: 4 (x_hi: 2, x_lo: 2; x = x_hi * 2 + x_lo), y: 4, z: 4, core: 2. Of those that a mesh axis runs over, the one named last changes fastest.
Arguments:
- image_hidden: bfloat16 [8, 4096, 3072], P('batch', 'seq', 'head'), parts along dimension 0, may hold values from -6 to 6
- modulation: float32 [8, 3, 3072], P('batch'), parts along dimension 0, may hold values from -4 to 4
- qkv_weight: bfloat16 [3072, 3, 1536], P(None, None, 'head'), may hold values from -0.109375 to 0.109375
- out_weight: bfloat16 [1536, 3072], P('head'), may hold values from -0.15625 to 0.15625
- q_gain: float32 [128], replicated, may hold values from 1.2 to 2.5
- k_gain: float32 [128], replicated, may hold values from 1.2 to 2.5
- text_keys: bfloat16 [8, 512, 1536], P('batch', 'seq', 'head'), parts along dimension 0, may hold values from -10 to 10
- text_values: bfloat16 [8, 512, 1536], P('batch', 'seq', 'head'), parts along dimension 0, may hold values from -6 to 6
- stale_keys: bfloat16 [8, 4096, 1536], P('batch', 'seq', 'head'), parts along dimension 0, may hold values from -64 to 64
- stale_values: bfloat16 [8, 4096, 1536], P('batch', 'seq', 'head'), parts along dimension 0, may hold values from -6 to 6
- cached_residual: bfloat16 [8, 4096, 3072], P('batch', 'seq', 'head'), parts along dimension 0, may hold values from -6 to 6
- patch_of: int32 [64], P('batch'), parts along dimension 0, may hold values from 0 to 15, each once
- refresh: int32 [64], P('batch'), parts along dimension 0, may hold values from 0 to 1, as said below
- text_len: int32 [8], P('batch'), parts along dimension 0, may hold values from 64 to 512
Outputs:
- image_out: bfloat16 [8, 4096, 3072], P('batch', 'seq', 'head'), parts along dimension 0
The draws below stay inside these ranges and needn't reach their ends.
There are 4 independent parts, one for each index of `batch`. The reference program is written for one: setup_inputs(seed, part) draws one part's arguments, and reference() takes and returns one part's arrays. A program takes and returns all parts, laid end to end along the dimension named above; an argument that names none is the same for every part. Nothing has to cross between parts.
Inputs may be any that keep to these rules, and one draw needn't show every extreme that they name: `patch_of`: A permutation: every image band sits on exactly one index of seq. `refresh`: exactly 4 entries are 1, the rest 0.
All inputs are finite; a program needn't handle non-finite values.
Results may differ from the reference program's by a relative error of at most 0.012.
The reference program's roundings to bfloat16 on the way count: a program that leaves them out, or rounds other values in their place, can miss the bound.
Values may be sent and summed in bfloat16 or wider, within the bound.
A program may use at most 192 MiB of HBM per device.

```python
import math
import jax
import jax.numpy as jnp
from jax import lax

D = 3072
HEADS = 12
HEAD_DIM = 128
GRID_W = 64
PROMPTS = 2
IMG_DEV = 256
IMG = 4096
TXT = 512
REFRESH = 4
N_SEQ = 16


def draw_stale_keys(key, part):
    shape = (PROMPTS, IMG, HEADS * HEAD_DIM)
    drawn = 1.8 * jax.random.truncated_normal(key, -5.0, 5.0, shape, jnp.float32)
    return drawn.astype(jnp.bfloat16)


def draw_refresh(key, part):
    shuffled = jax.random.permutation(key, N_SEQ)
    return (shuffled < REFRESH).astype(jnp.int32)


def steps_of(rng, shape, cuts, low, top_value):
    factor_of, own = 1.0, jax.random.fold_in(rng, 6)
    for dim, parts in cuts:
        heights = jnp.exp(jax.random.uniform(jax.random.fold_in(own, dim), (parts,), jnp.float32, low / len(cuts), top_value / len(cuts)))
        factor_of = factor_of * jnp.repeat(heights, shape[dim] // parts).reshape([-1 if axis == dim else 1 for axis in range(len(shape))])
    return factor_of


def bell_draw(own_key, extent, spread, limit, cuts=(), kind=jnp.bfloat16):
    level = steps_of(own_key, extent, cuts, -0.22, 0.18) if cuts else 1.0
    entries = jax.random.normal(own_key, extent, jnp.float32) * spread * level
    return jnp.minimum(jnp.maximum(entries, -limit), limit).astype(kind)


def setup_inputs(seed: int = 0, part: int = 0) -> dict:
    key_list = jax.random.split(jax.random.key(seed), 15)
    part_keys = jax.random.split(jax.random.fold_in(key_list[14], part), 15)
    image_hidden = bell_draw(part_keys[0], (PROMPTS, IMG, D), 1.0, 6.0, ((1, 16), (2, 2)))
    modulation = bell_draw(part_keys[1], (PROMPTS, 3, D), 0.8, 4.0, (), jnp.float32)
    qkv_weight = bell_draw(key_list[2], (D, 3, HEADS * HEAD_DIM), D ** -0.5, 0.109375, ((2, 2),))
    out_weight = bell_draw(key_list[3], (HEADS * HEAD_DIM, D), (HEADS * HEAD_DIM) ** -0.5, 0.15625, ((0, 2),))
    q_gain = jnp.clip(jnp.exp(jax.random.uniform(key_list[4], (HEAD_DIM,), jnp.float32, math.log(1.2), math.log(2.5))), 1.2, 2.5)
    k_gain = jnp.clip(jnp.exp(jax.random.uniform(key_list[5], (HEAD_DIM,), jnp.float32, math.log(1.2), math.log(2.5))), 1.2, 2.5)
    text_keys = bell_draw(part_keys[6], (PROMPTS, TXT, HEADS * HEAD_DIM), 1.8, 10.0, ((1, 16), (2, 2)))
    text_values = bell_draw(part_keys[7], (PROMPTS, TXT, HEADS * HEAD_DIM), 1.0, 6.0, ((1, 16), (2, 2)))
    stale_keys = draw_stale_keys(jax.random.fold_in(jax.random.fold_in(key_list[14], part), 71), part)
    stale_values = bell_draw(part_keys[9], (PROMPTS, IMG, HEADS * HEAD_DIM), 1.0, 6.0, ((1, 16), (2, 2)))
    cached_residual = bell_draw(part_keys[10], (PROMPTS, IMG, D), 1.0, 6.0, ((1, 16), (2, 2)))
    patch_of = jax.random.permutation(part_keys[11], N_SEQ).astype(jnp.int32)
    refresh = draw_refresh(jax.random.fold_in(jax.random.fold_in(key_list[14], part), 71), part)
    text_len = jax.random.randint(part_keys[13], (PROMPTS,), TXT // 8, TXT + 1).astype(jnp.int32)
    return dict(image_hidden=image_hidden, modulation=modulation, qkv_weight=qkv_weight, out_weight=out_weight, q_gain=q_gain, k_gain=k_gain, text_keys=text_keys, text_values=text_values, stale_keys=stale_keys, stale_values=stale_values, cached_residual=cached_residual, patch_of=patch_of, refresh=refresh, text_len=text_len)


epsilon = 1e-06

def rotary_tables(raster, head_dim, grid_width):
    half_dim = head_dim // 2
    first_pairs = head_dim // 16
    axis_pairs = (half_dim - first_pairs) // 2
    pair_index = jnp.arange(half_dim, dtype=jnp.int32)
    pair_local = jnp.where(pair_index < first_pairs + axis_pairs, pair_index - first_pairs, pair_index - first_pairs - axis_pairs)
    exponent = -pair_local.astype(jnp.float32) / float(axis_pairs)
    frequency = jnp.where(pair_index < first_pairs, jnp.float32(0.0), jnp.power(jnp.float32(10000.0), exponent))
    row_pos = (raster // grid_width).astype(jnp.float32)
    col_pos = (raster % grid_width).astype(jnp.float32)
    position = jnp.where(pair_index[None, :] < first_pairs + axis_pairs, row_pos[:, None], col_pos[:, None])
    angles = position * frequency[None, :]
    cosine = jnp.cos(angles)
    sine = jnp.sin(angles)
    return (jnp.concatenate([cosine, cosine], axis=-1), jnp.concatenate([-sine, sine], axis=-1))

def rms_rotate(vectors, gain_vec, cos_full, sin_full):
    scaled = vectors * lax.rsqrt(lax.optimization_barrier(jnp.mean(vectors * vectors, axis=-1, keepdims=True)) + epsilon) * gain_vec
    half_dim = vectors.shape[-1] // 2
    return scaled * cos_full[:, None, :] + jnp.roll(scaled, half_dim, axis=-1) * sin_full[:, None, :]

def reference(image_hidden, modulation, qkv_weight, out_weight, q_gain, k_gain, text_keys, text_values, stale_keys, stale_values, cached_residual, patch_of, refresh, text_len):
    channels = HEADS * HEAD_DIM
    hidden_f32 = image_hidden.astype(jnp.float32)
    row_mean = lax.optimization_barrier(jnp.mean(hidden_f32, axis=-1, keepdims=True))
    centered = hidden_f32 - row_mean
    variance = lax.optimization_barrier(jnp.mean(centered * centered, axis=-1, keepdims=True))
    normed = centered * lax.rsqrt(variance + epsilon)
    modulated = (normed * (1.0 + modulation[:, 1][:, None, :]) + modulation[:, 0][:, None, :]).astype(jnp.bfloat16)
    position = jnp.arange(IMG, dtype=jnp.int32)
    owner_seat = position // IMG_DEV
    raster = patch_of[owner_seat] * IMG_DEV + position % IMG_DEV
    cos_full, sin_full = rotary_tables(raster, HEAD_DIM, GRID_W)
    refreshed = refresh[owner_seat] == 1
    score_scale = HEAD_DIM ** (-0.5)
    results = []
    for prompt in range(PROMPTS):
        projected = jnp.dot(modulated[prompt], qkv_weight.reshape(D, 3 * channels), preferred_element_type=jnp.float32)
        projected = projected.reshape(IMG, 3, HEADS, HEAD_DIM)
        fresh_q = rms_rotate(projected[:, 0], q_gain, cos_full, sin_full).astype(jnp.bfloat16)
        fresh_k = rms_rotate(projected[:, 1], k_gain, cos_full, sin_full).astype(jnp.bfloat16)
        fresh_v = projected[:, 2].astype(jnp.bfloat16)
        stale_k = stale_keys[prompt].reshape(IMG, HEADS, HEAD_DIM)
        stale_v = stale_values[prompt].reshape(IMG, HEADS, HEAD_DIM)
        text_key_rows = text_keys[prompt].reshape(TXT, HEADS, HEAD_DIM)
        text_value_rows = text_values[prompt].reshape(TXT, HEADS, HEAD_DIM)
        key_mask = jnp.concatenate([jnp.arange(TXT, dtype=jnp.int32) < text_len[prompt], jnp.ones((IMG,), jnp.bool_)])

        def attend(seq_index):
            use_fresh = refreshed | (owner_seat == seq_index)
            key_rows = jnp.where(use_fresh[:, None, None], fresh_k, stale_k)
            value_rows = jnp.where(use_fresh[:, None, None], fresh_v, stale_v)
            all_keys = jnp.concatenate([text_key_rows, key_rows], axis=0)
            all_values = jnp.concatenate([text_value_rows, value_rows], axis=0)
            queries = lax.dynamic_slice_in_dim(fresh_q, seq_index * IMG_DEV, IMG_DEV, 0)
            scores = jnp.einsum('qhd,khd->hqk', queries.astype(jnp.float32), all_keys.astype(jnp.float32)) * score_scale
            scores = jnp.where(key_mask[None, None, :], scores, -1e+30)
            row_top = lax.optimization_barrier(jnp.max(scores, axis=-1, keepdims=True))
            weights = jnp.exp(scores - row_top)
            row_sums = lax.optimization_barrier(jnp.sum(weights, axis=-1))
            probs = weights.astype(jnp.bfloat16)
            numerator = jnp.einsum('hqk,khd->qhd', probs.astype(jnp.float32), all_values.astype(jnp.float32))
            return (numerator / jnp.transpose(row_sums)[:, :, None]).astype(jnp.bfloat16)
        attended = lax.map(attend, jnp.arange(N_SEQ, dtype=jnp.int32)).reshape(IMG, channels)
        projection = jnp.dot(attended, out_weight, preferred_element_type=jnp.float32)
        combined = hidden_f32[prompt] + modulation[prompt, 2][None, :] * projection + cached_residual[prompt].astype(jnp.float32)
        results.append(combined.astype(jnp.bfloat16))
    return jnp.stack(results, axis=0)
```

```python
import functools
import math

import jax
import jax.numpy as jnp
from jax import lax
from jax.experimental import pallas as pl
from jax.experimental.pallas import tpu as pltpu
from jax.sharding import PartitionSpec as P

GRID_W = 64
EPS = 1e-06
NEG = -1e30
MESH = pl.DeviceIdType.MESH
BF = jnp.bfloat16
F32 = jnp.float32

NC = 4
TRI = 3
RS = 6


def rotary_tables(raster, head_dim, grid_width):
    half_dim = head_dim // 2
    first_pairs = head_dim // 16
    axis_pairs = (half_dim - first_pairs) // 2
    pair_index = jnp.arange(half_dim, dtype=jnp.int32)
    pair_local = jnp.where(
        pair_index < first_pairs + axis_pairs,
        pair_index - first_pairs,
        pair_index - first_pairs - axis_pairs,
    )
    exponent = -pair_local.astype(jnp.float32) / float(axis_pairs)
    frequency = jnp.where(
        pair_index < first_pairs, jnp.float32(0.0), jnp.power(jnp.float32(10000.0), exponent)
    )
    row_pos = (raster // grid_width).astype(jnp.float32)
    col_pos = (raster % grid_width).astype(jnp.float32)
    position = jnp.where(
        pair_index[None, :] < first_pairs + axis_pairs, row_pos[:, None], col_pos[:, None]
    )
    angles = position * frequency[None, :]
    cosine = jnp.cos(angles)
    sine = jnp.sin(angles)
    return (jnp.concatenate([cosine, cosine], axis=-1), jnp.concatenate([-sine, sine], axis=-1))


def kernel(
    nb,
    refresh_ref,
    tlen_ref,
    mod_ref,
    cos_ref,
    sin_ref,
    qg_ref,
    kg_ref,
    x_hbm,
    w_hbm,
    wo_hbm,
    tk_hbm,
    tv_hbm,
    sk_hbm,
    sv_hbm,
    cr_hbm,
    out_hbm,
    w,
    xo,
    xp,
    xm,
    sk,
    sv,
    cr,
    stage,
    fresh,
    rowb,
    kvb,
    textb,
    acc,
    mst,
    lst,
    oown,
    mown,
    lown,
    osend,
    ob,
    attb,
    attp,
    wown,
    woth,
    pacc,
    outv,
    lsem,
    img_s,
    img_r,
    txt_s,
    txt_r,
    ty_s,
    ty_r,
    row_s,
    row_r,
    y_s,
    y_r,
    f_s,
    f_r,
    o_s,
    o_r,
    a_s,
    a_r,
    w_s,
    w_r,
):
    b = lax.axis_index("batch")
    me = lax.axis_index("seq")
    h = lax.axis_index("head")
    k = me % 2
    xl = (me // 2) % 2
    y = me // 4
    mine = me % 4
    half = xo.shape[2]
    width = 2 * half
    cr_rows = xo.shape[1] // NC
    hd = 128
    tw = TRI * hd
    ns = 2 * nb
    wrows = woth.shape[0] // ns
    trow = tk_hbm.shape[1]
    cexp = (hd ** -0.5) * math.log2(math.e)

    def member(rel):
        return ((xl + rel // 2) % 2) * 2 + (k + rel % 2) % 2

    def row_peer(rel):
        return {"seq": y * 4 + member(rel)}

    def y_of(d):
        return (y + d) % 4

    def y_peer(d):
        return {"seq": y_of(d) * 4 + mine}

    partner = {"head": 1 - h}

    def remote(src, dst, ss, rs, dev):
        return pltpu.make_async_remote_copy(src, dst, ss, rs, device_id=dev, device_id_type=MESH)

    local = [
        pltpu.make_async_copy(x_hbm, xo, lsem.at[0]),
        pltpu.make_async_copy(w_hbm.at[0], w.at[0], lsem.at[1]),
        pltpu.make_async_copy(w_hbm.at[1], w.at[1], lsem.at[2]),
        pltpu.make_async_copy(w_hbm.at[2], w.at[2], lsem.at[3]),
        pltpu.make_async_copy(sk_hbm, sk, lsem.at[4]),
        pltpu.make_async_copy(sv_hbm, sv, lsem.at[5]),
        pltpu.make_async_copy(
            wo_hbm.at[:, pl.ds(pl.multiple_of(h * half, 128), half)], wown, lsem.at[6]
        ),
        pltpu.make_async_copy(cr_hbm, cr, lsem.at[7]),
    ]
    for c_ in local:
        c_.start()

    peers = [partner]
    peers += [row_peer(r) for r in (1, 2, 3)]
    peers += [y_peer(d) for d in (1, 2, 3)]
    zpeers = []
    for db in range(nb):
        for dk in range(2):
            if db == 0 and dk == 0:
                continue
            dev = {"batch": (b + db) % nb, "seq": me + dk * (1 - 2 * k)}
            zpeers.append((db, dk, dev))
            if db != 0:
                peers.append(dev)
    bar = pltpu.get_barrier_semaphore()
    for p_ in peers:
        pl.semaphore_signal(bar, inc=1, device_id=p_, device_id_type=MESH)
    pl.semaphore_wait(bar, len(peers))

    def img(c):
        rows = pl.ds(pl.multiple_of(c * cr_rows, cr_rows), cr_rows)
        return remote(x_hbm.at[:, rows], xp.at[:, rows], img_s.at[c], img_r.at[c], partner)

    img(0).start()
    img(1).start()

    def txt(rel, part):
        m = member(rel)
        src = (tk_hbm if part == 0 else tv_hbm).at[
            m // 2, :, pl.ds(pl.multiple_of((m % 2) * tw, 128), tw)
        ]
        dst = textb.at[y, mine, :, pl.ds(part * tw, tw)]
        return src, dst

    def txt_remote(rel, part):
        src, dst = txt(rel, part)
        return remote(src, dst, txt_s.at[rel, part], txt_r.at[rel, part], row_peer(rel))

    def txt_arrival(rel, part):
        landed = textb.at[y, member(rel), :, pl.ds(part * tw, tw)]
        return remote(landed, landed, txt_s.at[rel, part], txt_r.at[rel, part], row_peer(rel))

    own_text = []
    for part in range(2):
        src, dst = txt(0, part)
        cp = pltpu.make_async_copy(src, dst, lsem.at[8 + part])
        cp.start()
        own_text.append(cp)
    for rel in (2, 3, 1):
        for part in range(2):
            txt_remote(rel, part).start()

    def row_send(c, rel):
        m = member(rel)
        return remote(
            stage.at[c, m], rowb.at[mine, c], row_s.at[c, rel], row_r.at[c, rel], row_peer(rel)
        )

    def row_arrival(c, rel):
        m = member(rel)
        return remote(
            rowb.at[m, c], rowb.at[m, c], row_s.at[c, rel], row_r.at[c, rel], row_peer(rel)
        )

    def pair_of(part):
        return pl.ds(2 * ((xl + part) % 2), 2)

    def y_send(c, part, way):
        d = 1 if way == 0 else 3
        return remote(
            rowb.at[pair_of(part), c, :, pl.ds(tw, 2 * tw)],
            kvb.at[y, c, pair_of(part)],
            y_s.at[c, part, way],
            y_r.at[c, part, way],
            y_peer(d),
        )

    def y_arrival(c, part, way):
        d = 3 if way == 0 else 1
        landed = kvb.at[y_of(d), c, pair_of(part)]
        return remote(landed, landed, y_s.at[c, part, way], y_r.at[c, part, way], y_peer(d))

    def fwd(c, part):
        d_from = 3 if part == 0 else 1
        d_to = 1 if part == 0 else 3
        held = kvb.at[y_of(d_from), c, pair_of(part)]
        return remote(held, held, f_s.at[c, part], f_r.at[c, part], y_peer(d_to))

    def fwd_arrival(c, part):
        d_from = 3 if part == 0 else 1
        landed = kvb.at[y_of(2), c, pair_of(part)]
        return remote(landed, landed, f_s.at[c, part], f_r.at[c, part], y_peer(d_from))

    def serve_a(c):
        row_arrival(c, 1).wait_recv()
        for way in range(2):
            y_send(c, 0, way).start()

    def serve_b(c):
        row_arrival(c, 2).wait_recv()
        row_arrival(c, 3).wait_recv()
        for way in range(2):
            y_send(c, 1, way).start()

    def forward_a(c):
        y_arrival(c, 0, 0).wait_recv()
        fwd(c, 0).start()

    def forward_b(c):
        y_arrival(c, 1, 1).wait_recv()
        fwd(c, 1).start()

    flag = refresh_ref[me]
    own_off = pl.multiple_of(h * half, 128)
    part_off = pl.multiple_of((1 - h) * half, 128)

    for c_ in local[:6]:
        c_.wait()

    def qkv_step(c, carry):
        img(c).wait_recv()
        rows = pl.ds(pl.multiple_of(c * cr_rows, cr_rows), cr_rows)
        for p in range(2):
            a = xo[p, rows, :].astype(F32)
            d = xp[p, rows, :].astype(F32)
            total = jnp.sum(a, axis=-1, keepdims=True) + jnp.sum(d, axis=-1, keepdims=True)
            mean = total / width
            a = a - mean
            d = d - mean
            var = (
                jnp.sum(a * a, axis=-1, keepdims=True) + jnp.sum(d * d, axis=-1, keepdims=True)
            ) / width
            inv = lax.rsqrt(var + EPS)
            for i, (v, off) in enumerate(((a, own_off), (d, part_off))):
                scale = 1.0 + mod_ref[1, pl.ds(p, 1), pl.ds(off, half)]
                shift = mod_ref[0, pl.ds(p, 1), pl.ds(off, half)]
                xm[i, pl.ds(p * cr_rows, cr_rows), :] = (v * inv * scale + shift).astype(BF)
        cosv = cos_ref[rows, :]
        sinv = sin_ref[rows, :]
        cosv = jnp.concatenate([cosv, cosv], axis=0)
        sinv = jnp.concatenate([sinv, sinv], axis=0)
        for kind in range(3):
            proj = jnp.dot(
                xm[0], w[kind, pl.ds(own_off, half), :], preferred_element_type=F32
            ) + jnp.dot(xm[1], w[kind, pl.ds(part_off, half), :], preferred_element_type=F32)
            for head in range(2 * TRI):
                t = proj[:, head * hd : (head + 1) * hd]
                if kind < 2:
                    gain = (qg_ref if kind == 0 else kg_ref)[...]
                    ms = jnp.mean(t * t, axis=-1, keepdims=True)
                    t = t * lax.rsqrt(ms + EPS) * gain
                    t = t * cosv + pltpu.roll(t, hd // 2, 1) * sinv
                t = t.astype(BF)
                kk, j = head // TRI, head % TRI
                for p in range(2):
                    m = p * 2 + kk
                    piece = t[p * cr_rows : (p + 1) * cr_rows]
                    if kind == 0:
                        stage[c, m, :, j * hd : (j + 1) * hd] = piece
                    else:
                        fresh[c, m, :, (kind - 1) * tw + j * hd : (kind - 1) * tw + (j + 1) * hd] = (
                            piece
                        )
                        old = (sk if kind == 1 else sv)[p, rows, head * hd : (head + 1) * hd]
                        stage[c, m, :, kind * tw + j * hd : kind * tw + (j + 1) * hd] = jnp.where(
                            flag == 1, piece, old
                        )
        for rel in (2, 3, 1):
            row_send(c, rel).start()

        @pl.when(c + 2 < NC)
        def _():
            img(c + 2).start()

        rowb[mine, c] = stage[c, mine]
        serve_a(c)

        @pl.when(c >= 1)
        def _():
            serve_b(c - 1)
            forward_a(c - 1)

        @pl.when(c >= 2)
        def _():
            forward_b(c - 2)

        return carry

    lax.fori_loop(0, NC, qkv_step, 0)

    for cp in own_text:
        cp.wait()
    for rel in (1, 2, 3):
        for part in range(2):
            txt_arrival(rel, part).wait_recv()

    def ty(d):
        return remote(textb.at[y], textb.at[y], ty_s.at[d - 1], ty_r.at[d - 1], y_peer(d))

    def ty_arrival(d):
        landed = textb.at[y_of(4 - d)]
        return remote(landed, landed, ty_s.at[d - 1], ty_r.at[d - 1], y_peer(4 - d))

    for d in (1, 2, 3):
        ty(d).start()

    def w_slot(db, dk):
        return ((b + nb - db) % nb) * 2 + (k + dk) % 2

    def w_rows(s):
        return pl.ds(pl.multiple_of(s * wrows, wrows), wrows)

    my_rows = w_rows(b * 2 + k)
    w_first = remote(
        wo_hbm.at[my_rows, pl.ds(part_off, half)],
        woth.at[my_rows],
        w_s.at[0],
        w_r.at[0],
        partner,
    )
    w_first.start()

    def update(q, blocks, first, m_old, l_old, a_old):
        scores = []
        for kb, _, mask in blocks:
            s = lax.dot_general(
                q, kb(), (((1,), (1,)), ((), ())), preferred_element_type=F32
            )
            if mask is not None:
                s = jnp.where(mask(s.shape), s, NEG)
            scores.append(s)
        top = scores[0]
        top = jnp.max(top, axis=-1, keepdims=True)
        for s in scores[1:]:
            top = jnp.maximum(top, jnp.max(s, axis=-1, keepdims=True))
        if not first:
            top = jnp.maximum(top, m_old)
        ref = top * cexp
        a_new = None
        l_new = None
        for s, (_, vb, _) in zip(scores, blocks):
            e = jnp.exp2(s * cexp - ref)
            ls = jnp.sum(e, axis=-1, keepdims=True)
            av = jnp.dot(e.astype(BF), vb(), preferred_element_type=F32)
            l_new = ls if l_new is None else l_new + ls
            a_new = av if a_new is None else a_new + av
        if not first:
            shrink = jnp.exp2(m_old * cexp - ref)
            l_new = l_new + l_old * shrink
            a_new = a_new + a_old * shrink
        return top, l_new, a_new

    nrow = NC * cr_rows

    def own_step(m, carry):
        for j in range(TRI):
            q = stage[:, m, :, j * hd : (j + 1) * hd].reshape(nrow, hd)

            def kb():
                return fresh[:, m, :, j * hd : (j + 1) * hd].reshape(nrow, hd)

            def vb():
                return fresh[:, m, :, tw + j * hd : tw + (j + 1) * hd].reshape(nrow, hd)

            top, tot, av = update(q, [(kb, vb, None)], True, None, None, None)
            oown[m, j] = av
            mown[m, j] = jnp.broadcast_to(top, (nrow, hd))
            lown[m, j] = jnp.broadcast_to(tot, (nrow, hd))
        return carry

    lax.fori_loop(0, 4, own_step, 0)

    forward_b(NC - 2)
    serve_b(NC - 1)
    forward_a(NC - 1)

    for d in (1, 2, 3):
        ty_arrival(d).wait_recv()
    tlen = tlen_ref[xl]

    def text_and_row(m, carry):
        for j in range(TRI):
            q = rowb[m, :, :, j * hd : (j + 1) * hd].reshape(nrow, hd)
            blocks = []
            for t in range(2):

                def kb(t=t):
                    return textb[2 * t : 2 * t + 2, :, :, j * hd : (j + 1) * hd].reshape(
                        8 * trow, hd
                    )

                def vb(t=t):
                    return textb[2 * t : 2 * t + 2, :, :, tw + j * hd : tw + (j + 1) * hd].reshape(
                        8 * trow, hd
                    )

                def mask(shape, t=t):
                    return lax.broadcasted_iota(jnp.int32, shape, 1) + t * 8 * trow < tlen

                blocks.append((kb, vb, mask))
            for c in range(NC):

                def kb(c=c):
                    return rowb[:, c, :, tw + j * hd : tw + (j + 1) * hd].reshape(4 * cr_rows, hd)

                def vb(c=c):
                    return rowb[:, c, :, 2 * tw + j * hd : 2 * tw + (j + 1) * hd].reshape(
                        4 * cr_rows, hd
                    )

                def mask(shape):
                    return lax.broadcasted_iota(jnp.int32, shape, 1) // cr_rows != m

                blocks.append((kb, vb, mask))
            top, tot, av = update(q, blocks, True, None, None, None)
            acc[m, j] = av
            mst[m, j] = jnp.broadcast_to(top, (nrow, hd))
            lst[m, j] = jnp.broadcast_to(tot, (nrow, hd))
        return carry

    lax.fori_loop(0, 4, text_and_row, 0)

    forward_b(NC - 1)

    remote(woth.at[my_rows], woth.at[my_rows], w_s.at[0], w_r.at[0], partner).wait_recv()
    for i, (db, dk, dev) in enumerate(zpeers):
        remote(woth.at[my_rows], woth.at[my_rows], w_s.at[1 + i], w_r.at[1 + i], dev).start()

    def far_blocks(ys, j):
        blocks = []
        for c in range(NC):

            def kb(c=c):
                return kvb[ys, c, :, :, j * hd : (j + 1) * hd].reshape(4 * cr_rows, hd)

            def vb(c=c):
                return kvb[ys, c, :, :, tw + j * hd : tw + (j + 1) * hd].reshape(4 * cr_rows, hd)

            blocks.append((kb, vb, None))
        return blocks

    def far(ys, m, last):
        res = []
        for j in range(TRI):
            q = rowb[m, :, :, j * hd : (j + 1) * hd].reshape(nrow, hd)
            top, tot, av = update(
                q, far_blocks(ys, j), False, mst[m, j][:, :1], lst[m, j][:, :1], acc[m, j]
            )
            if last:
                res.append((top, tot, av))
            else:
                acc[m, j] = av
                mst[m, j] = jnp.broadcast_to(top, (nrow, hd))
                lst[m, j] = jnp.broadcast_to(tot, (nrow, hd))
        return res

    def far_step(ys):
        def step(m, carry):
            far(ys, m, False)
            return carry

        lax.fori_loop(0, 4, step, 0)

    for c in range(NC):
        y_arrival(c, 1, 0).wait_recv()
    far_step(y_of(3))
    for c in range(NC):
        y_arrival(c, 0, 1).wait_recv()
    far_step(y_of(1))
    for c in range(NC):
        fwd_arrival(c, 0).wait_recv()
        fwd_arrival(c, 1).wait_recv()

    lane = lax.broadcasted_iota(jnp.int32, (nrow, hd), 1)

    def o_send(rel):
        m = member(rel)
        return remote(osend.at[m], ob.at[mine], o_s.at[rel], o_r.at[rel], row_peer(rel))

    def o_arrival(rel):
        m = member(rel)
        return remote(ob.at[m], ob.at[m], o_s.at[rel], o_r.at[rel], row_peer(rel))

    def last_step(i, carry):
        rel = 3 - i
        m = member(rel)
        stats = jnp.zeros((nrow, hd), F32)
        for j, (top, tot, av) in enumerate(far(y_of(2), m, True)):
            osend[m, :, j * hd : (j + 1) * hd] = (av / tot).astype(BF)
            for idx, val in ((2 * j, top), (2 * j + 1, tot)):
                hi = val.astype(BF).astype(F32)
                rest = val - hi
                mid = rest.astype(BF).astype(F32)
                low = rest - mid
                stats = jnp.where(lane == idx, hi, stats)
                stats = jnp.where(lane == RS + idx, mid, stats)
                stats = jnp.where(lane == 2 * RS + idx, low, stats)
        osend[m, :, tw : tw + hd] = stats.astype(BF)

        @pl.when(rel > 0)
        def _():
            o_send(rel).start()

        return carry

    lax.fori_loop(0, 4, last_step, 0)
    ob[mine] = osend[mine]

    def a_send(m):
        return remote(attb.at[m], attp.at[m], a_s.at[m], a_r.at[m], partner)

    def merge(rel, carry):
        m = member(rel)

        @pl.when(rel > 0)
        def _():
            o_arrival(rel).wait_recv()

        stats = ob[m, :, tw : tw + hd].astype(F32)
        for j in range(TRI):

            def col(idx):
                return (
                    stats[:, idx : idx + 1]
                    + stats[:, RS + idx : RS + idx + 1]
                    + stats[:, 2 * RS + idx : 2 * RS + idx + 1]
                )

            m1, l1 = col(2 * j), col(2 * j + 1)
            m2, l2 = mown[m, j][:, :1], lown[m, j][:, :1]
            top = jnp.maximum(m1, m2)
            w1 = l1 * jnp.exp2((m1 - top) * cexp)
            e2 = jnp.exp2((m2 - top) * cexp)
            den = w1 + l2 * e2
            o1 = ob[m, :, j * hd : (j + 1) * hd].astype(F32)
            attb[m, :, j * hd : (j + 1) * hd] = (
                o1 * (w1 / den) + oown[m, j] * (e2 / den)
            ).astype(BF)
        a_send(m).start()
        return carry

    lax.fori_loop(0, 4, merge, 0)

    local[6].wait()
    local[7].wait()
    for i, (db, dk, dev) in enumerate(zpeers):
        rows = w_rows(w_slot(db, dk))
        remote(woth.at[rows], woth.at[rows], w_s.at[1 + i], w_r.at[1 + i], dev).wait_recv()

    def own_proj(p, carry):
        pacc[p] = jnp.dot(attb[2 * p], wown[0:tw, :], preferred_element_type=F32) + jnp.dot(
            attb[2 * p + 1], wown[tw : 2 * tw, :], preferred_element_type=F32
        )
        return carry

    lax.fori_loop(0, 2, own_proj, 0)

    def finish(i, carry):
        p = (xl + i) % 2
        for kk in range(2):
            m = 2 * p + kk
            remote(attp.at[m], attp.at[m], a_s.at[m], a_r.at[m], partner).wait_recv()
        proj = (
            pacc[p]
            + jnp.dot(attp[2 * p], woth[0:tw, :], preferred_element_type=F32)
            + jnp.dot(attp[2 * p + 1], woth[tw : 2 * tw, :], preferred_element_type=F32)
        )
        gate = mod_ref[2, pl.ds(p, 1), pl.ds(own_off, half)]
        outv[p] = (xo[p].astype(F32) + gate * proj + cr[p].astype(F32)).astype(BF)
        pltpu.make_async_copy(outv.at[p], out_hbm.at[p], lsem.at[10 + i]).start()
        return carry

    lax.fori_loop(0, 2, finish, 0)

    for i in range(2):
        p = (xl + i) % 2
        pltpu.make_async_copy(outv.at[p], out_hbm.at[p], lsem.at[10 + i]).wait()
    for c in range(NC):
        img(c).wait_send()
        for rel in (1, 2, 3):
            row_send(c, rel).wait_send()
        for part in range(2):
            for way in range(2):
                y_send(c, part, way).wait_send()
            fwd(c, part).wait_send()
    for rel in (1, 2, 3):
        for part in range(2):
            txt_remote(rel, part).wait_send()
        o_send(rel).wait_send()
    for d in (1, 2, 3):
        ty(d).wait_send()
    w_first.wait_send()
    for i, (db, dk, dev) in enumerate(zpeers):
        remote(woth.at[my_rows], woth.at[my_rows], w_s.at[1 + i], w_r.at[1 + i], dev).wait_send()
    for m in range(4):
        a_send(m).wait_send()


def per_device(
    nb,
    image_hidden,
    modulation,
    qkv_weight,
    out_weight,
    q_gain,
    k_gain,
    text_keys,
    text_values,
    stale_keys,
    stale_values,
    cached_residual,
    patch_of,
    refresh,
    text_len,
):
    prompts, rows, half = image_hidden.shape
    hd = q_gain.shape[0]
    channels = out_weight.shape[0]
    tw = TRI * hd
    cr_rows = rows // NC
    trow = text_keys.shape[1]
    seat = lax.axis_index("seq")
    seat_ids = jnp.arange(patch_of.shape[0], dtype=jnp.int32)
    own_band = jnp.sum(jnp.where(seat_ids == seat, patch_of, 0))
    raster = own_band * rows + jnp.arange(rows, dtype=jnp.int32)
    cos_full, sin_full = rotary_tables(raster, hd, GRID_W)
    smem = pl.BlockSpec(memory_space=pltpu.SMEM)
    vmem = pl.BlockSpec(memory_space=pltpu.VMEM)
    hbm = pl.BlockSpec(memory_space=pl.ANY)
    dma = pltpu.SemaphoreType.DMA
    ns = 2 * nb
    return pl.pallas_call(
        functools.partial(kernel, nb),
        name="joint",
        out_shape=jax.ShapeDtypeStruct(image_hidden.shape, BF),
        in_specs=[smem, smem] + [vmem] * 5 + [hbm] * 8,
        out_specs=hbm,
        scratch_shapes=[
            pltpu.VMEM((3, 2 * half, channels), BF),
            pltpu.VMEM((prompts, rows, half), BF),
            pltpu.VMEM((prompts, rows, half), BF),
            pltpu.VMEM((2, prompts * cr_rows, half), BF),
            pltpu.VMEM((prompts, rows, channels), BF),
            pltpu.VMEM((prompts, rows, channels), BF),
            pltpu.VMEM((prompts, rows, half), BF),
            pltpu.VMEM((NC, 4, cr_rows, 3 * tw), BF),
            pltpu.VMEM((NC, 4, cr_rows, 2 * tw), BF),
            pltpu.VMEM((4, NC, cr_rows, 3 * tw), BF),
            pltpu.VMEM((4, NC, 4, cr_rows, 2 * tw), BF),
            pltpu.VMEM((4, 4, trow, 2 * tw), BF),
            pltpu.VMEM((4, TRI, rows, hd), F32),
            pltpu.VMEM((4, TRI, rows, hd), F32),
            pltpu.VMEM((4, TRI, rows, hd), F32),
            pltpu.VMEM((4, TRI, rows, hd), F32),
            pltpu.VMEM((4, TRI, rows, hd), F32),
            pltpu.VMEM((4, TRI, rows, hd), F32),
            pltpu.VMEM((4, rows, tw + hd), BF),
            pltpu.VMEM((4, rows, tw + hd), BF),
            pltpu.VMEM((4, rows, tw), BF),
            pltpu.VMEM((4, rows, tw), BF),
            pltpu.VMEM((channels, half), BF),
            pltpu.VMEM((channels, half), BF),
            pltpu.VMEM((prompts, rows, half), F32),
            pltpu.VMEM((prompts, rows, half), BF),
            dma((12,)),
            dma((NC,)),
            dma((NC,)),
            dma((4, 2)),
            dma((4, 2)),
            dma((3,)),
            dma((3,)),
            dma((NC, 4)),
            dma((NC, 4)),
            dma((NC, 2, 2)),
            dma((NC, 2, 2)),
            dma((NC, 2)),
            dma((NC, 2)),
            dma((4,)),
            dma((4,)),
            dma((4,)),
            dma((4,)),
            dma((ns,)),
            dma((ns,)),
        ],
        compiler_params=pltpu.CompilerParams(
            collective_id=0, has_side_effects=True, vmem_limit_bytes=66 * 1024 * 1024 - 2097152
        ),
    )(
        refresh,
        text_len,
        jnp.transpose(modulation, (1, 0, 2)),
        cos_full,
        sin_full,
        q_gain.reshape(1, hd),
        k_gain.reshape(1, hd),
        image_hidden,
        jnp.transpose(qkv_weight, (1, 0, 2)),
        out_weight,
        text_keys,
        text_values,
        stale_keys,
        stale_values,
        cached_residual,
    )


def solution(mesh):
    in_specs = (
        P("batch", "seq", "head"),
        P("batch", None, None),
        P(None, None, "head"),
        P("head", None),
        P(),
        P(),
        P("batch", "seq", "head"),
        P("batch", "seq", "head"),
        P("batch", "seq", "head"),
        P("batch", "seq", "head"),
        P("batch", "seq", "head"),
        P("batch"),
        P("batch"),
        P("batch"),
    )
    out_specs = P("batch", "seq", "head")
    return jax.shard_map(
        functools.partial(per_device, mesh.shape["batch"]),
        mesh=mesh,
        in_specs=in_specs,
        out_specs=out_specs,
        check_vma=False,
    )
```

```python
import functools
import math

import jax
import jax.numpy as jnp
from jax import lax
from jax.experimental import pallas as pl
from jax.experimental.pallas import tpu as pltpu
from jax.sharding import PartitionSpec as P

EPS = 1e-06
NEG = -1e30
MESH = pl.DeviceIdType.MESH
BF = jnp.bfloat16
F32 = jnp.float32

NC = 4
TRI = 3


def pair_frequency(head_dim):
    half_dim = head_dim // 2
    first_pairs = head_dim // 16
    axis_pairs = (half_dim - first_pairs) // 2
    pair_index = jnp.arange(half_dim, dtype=jnp.int32)
    pair_local = jnp.where(
        pair_index < first_pairs + axis_pairs,
        pair_index - first_pairs,
        pair_index - first_pairs - axis_pairs,
    )
    exponent = -pair_local.astype(jnp.float32) / float(axis_pairs)
    frequency = jnp.where(
        pair_index < first_pairs, jnp.float32(0.0), jnp.power(jnp.float32(10000.0), exponent)
    )
    return jnp.concatenate([frequency, frequency]).reshape(1, head_dim)


def kernel(
    nb,
    patch_ref,
    refresh_ref,
    tlen_ref,
    mod_ref,
    freq_ref,
    qg_ref,
    kg_ref,
    x_hbm,
    w_hbm,
    wo_hbm,
    tk_hbm,
    tv_hbm,
    sk_hbm,
    sv_hbm,
    cr_hbm,
    out_hbm,
    w,
    xf,
    xo,
    cr,
    xm,
    stb,
    fresh,
    rowb,
    kvb,
    textb,
    acc,
    mst,
    lst,
    osend,
    att,
    wown,
    woth,
    outv,
    lsem,
    img_s,
    img_r,
    sib_s,
    sib_r,
    st_s,
    st_r,
    txt_s,
    txt_r,
    ty_s,
    ty_r,
    y_s,
    y_r,
    f_s,
    f_r,
    a_s,
    a_r,
    w_s,
    w_r,
):
    b = lax.axis_index("batch")
    me = lax.axis_index("seq")
    h = lax.axis_index("head")
    k = me % 2
    xl = (me // 2) % 2
    y = me // 4
    mine = me % 4
    half = xo.shape[2]
    width = 2 * half
    cr_rows = xo.shape[1] // NC
    tile = 4 * cr_rows
    hd = 128
    tw = TRI * hd
    ns = 2 * nb
    wrows = woth.shape[0] // ns
    trow = tk_hbm.shape[1]
    cexp = (hd ** -0.5) * math.log2(math.e)

    def member(rel):
        return ((xl + rel // 2) % 2) * 2 + (k + rel % 2) % 2

    def row_peer(rel, other=0):
        return {"seq": y * 4 + member(rel), "head": (h + other) % 2}

    def y_of(d):
        return (y + d) % 4

    def y_peer(d):
        return {"seq": y_of(d) * 4 + mine}

    partner = {"head": 1 - h}

    def remote(src, dst, ss, rs, dev):
        return pltpu.make_async_remote_copy(src, dst, ss, rs, device_id=dev, device_id_type=MESH)

    def rows_of(c):
        return pl.ds(pl.multiple_of(c * cr_rows, cr_rows), cr_rows)

    def tri_cols(kk):
        return pl.ds(pl.multiple_of(kk * tw, 128), tw)

    own_off = pl.multiple_of(h * half, 128)
    part_off = pl.multiple_of((1 - h) * half, 128)

    local = [
        pltpu.make_async_copy(x_hbm.at[xl], xf.at[h, mine], lsem.at[0]),
        pltpu.make_async_copy(sk_hbm.at[xl, :, tri_cols(k)], stb.at[mine, :, 0:tw], lsem.at[1]),
        pltpu.make_async_copy(
            sv_hbm.at[xl, :, tri_cols(k)], stb.at[mine, :, tw : 2 * tw], lsem.at[2]
        ),
        pltpu.make_async_copy(
            tk_hbm.at[xl, :, tri_cols(k)], textb.at[y, mine, :, 0:tw], lsem.at[3]
        ),
        pltpu.make_async_copy(
            tv_hbm.at[xl, :, tri_cols(k)], textb.at[y, mine, :, tw : 2 * tw], lsem.at[4]
        ),
    ]
    for kind in range(3):
        local.append(
            pltpu.make_async_copy(
                w_hbm.at[kind, :, tri_cols(k)], w.at[:, kind * tw : (kind + 1) * tw], lsem.at[5 + kind]
            )
        )
    late = [
        pltpu.make_async_copy(wo_hbm.at[:, pl.ds(own_off, half)], wown, lsem.at[8]),
        pltpu.make_async_copy(cr_hbm, cr, lsem.at[9]),
        pltpu.make_async_copy(x_hbm, xo, lsem.at[10]),
    ]
    for c_ in local:
        c_.start()

    peers = [row_peer(r, 1) for r in range(4)]
    peers += [row_peer(r) for r in (1, 2, 3)]
    peers += [y_peer(d) for d in (1, 2, 3)]
    zpeers = []
    for db in range(nb):
        for dk in range(2):
            if db == 0 and dk == 0:
                continue
            dev = {"batch": (b + db) % nb, "seq": me + dk * (1 - 2 * k)}
            zpeers.append((db, dk, dev))
            if db != 0:
                peers.append(dev)
    bar = pltpu.get_barrier_semaphore()
    for p_ in peers:
        pl.semaphore_signal(bar, inc=1, device_id=p_, device_id_type=MESH)
    pl.semaphore_wait(bar, len(peers))

    def txt(rel, part):
        m = member(rel)
        return remote(
            (tk_hbm if part == 0 else tv_hbm).at[m // 2, :, tri_cols(m % 2)],
            textb.at[y, mine, :, part * tw : (part + 1) * tw],
            txt_s.at[rel, part],
            txt_r.at[rel, part],
            row_peer(rel),
        )

    def txt_arrival(rel, part):
        landed = textb.at[y, member(rel), :, part * tw : (part + 1) * tw]
        return remote(landed, landed, txt_s.at[rel, part], txt_r.at[rel, part], row_peer(rel))

    def img_peer(kind):
        return row_peer((1, 0, 2, 2)[kind], (0, 1, 0, 1)[kind])

    def img(c, kind):
        p = xl if kind < 2 else 1 - xl
        return remote(
            x_hbm.at[p, rows_of(c)],
            xf.at[h, mine, rows_of(c)],
            img_s.at[c, kind],
            img_r.at[c, kind],
            img_peer(kind),
        )

    def img_landed(c, kind):
        m = member((1, 0, 2, 2)[kind])
        return xf.at[(h + (0, 1, 0, 1)[kind]) % 2, m, rows_of(c)]

    def img_arrival(c, kind):
        d = img_landed(c, kind)
        return remote(d, d, img_s.at[c, kind], img_r.at[c, kind], img_peer(kind))

    def pass_on(c, kind):
        d = img_landed(c, kind)
        return remote(d, d, sib_s.at[c, kind - 1], sib_r.at[c, kind - 1], row_peer(1))

    def pass_arrival(c, kind):
        m = member((1, 1, 3, 3)[kind])
        d = xf.at[(h + (0, 1, 0, 1)[kind]) % 2, m, rows_of(c)]
        return remote(d, d, sib_s.at[c, kind - 1], sib_r.at[c, kind - 1], row_peer(1))

    def stale(c, rel, part):
        m = member(rel)
        return remote(
            (sk_hbm if part == 0 else sv_hbm).at[m // 2, rows_of(c), tri_cols(m % 2)],
            stb.at[mine, rows_of(c), part * tw : (part + 1) * tw],
            st_s.at[c, rel, part],
            st_r.at[c, rel, part],
            row_peer(rel),
        )

    def stale_arrival(c, rel, part):
        d = stb.at[member(rel), rows_of(c), part * tw : (part + 1) * tw]
        return remote(d, d, st_s.at[c, rel, part], st_r.at[c, rel, part], row_peer(rel))

    def send_image(c):
        for kind in (1, 2, 3, 0):
            img(c, kind).start()

    def send_stale(c):
        for rel in (2, 3, 1):
            for part in range(2):
                stale(c, rel, part).start()

    send_image(0)
    for rel in (2, 3, 1):
        for part in range(2):
            txt(rel, part).start()
    send_stale(0)

    def send_chunk(c, carry):
        send_image(c)
        send_stale(c)
        return carry

    lax.fori_loop(1, NC, send_chunk, 0)

    def w_slot(db, dk):
        return ((b + nb - db) % nb) * 2 + (k + dk) % 2

    def w_rows(s):
        return pl.ds(pl.multiple_of(s * wrows, wrows), wrows)

    my_rows = w_rows(b * 2 + k)

    def w_pass(i):
        return remote(
            woth.at[my_rows], woth.at[my_rows], w_s.at[1 + i], w_r.at[1 + i], zpeers[i][2]
        )

    w_first = remote(
        wo_hbm.at[my_rows, pl.ds(part_off, half)],
        woth.at[my_rows],
        w_s.at[0],
        w_r.at[0],
        partner,
    )
    w_first.start()
    for c_ in late:
        c_.start()

    def ty(d):
        return remote(textb.at[y], textb.at[y], ty_s.at[d - 1], ty_r.at[d - 1], y_peer(d))

    def ty_arrival(d):
        landed = textb.at[y_of(4 - d)]
        return remote(landed, landed, ty_s.at[d - 1], ty_r.at[d - 1], y_peer(4 - d))

    for c_ in local:
        c_.wait()
    for rel in (1, 2, 3):
        for part in range(2):
            txt_arrival(rel, part).wait_recv()
    for d in (1, 3, 2):
        ty(d).start()

    def pair_of(part):
        return pl.ds(2 * ((xl + part) % 2), 2)

    def y_send(c, part, way):
        return remote(
            rowb.at[pair_of(part), c, :, tw : 3 * tw],
            kvb.at[y, c, pair_of(part)],
            y_s.at[c, part, way],
            y_r.at[c, part, way],
            y_peer(1 if way == 0 else 3),
        )

    def y_arrival(c, part, way):
        d = 3 if way == 0 else 1
        landed = kvb.at[y_of(d), c, pair_of(part)]
        return remote(landed, landed, y_s.at[c, part, way], y_r.at[c, part, way], y_peer(d))

    def fwd(c, part):
        held = kvb.at[y_of(3 if part == 0 else 1), c, pair_of(part)]
        return remote(
            held, held, f_s.at[c, part], f_r.at[c, part], y_peer(1 if part == 0 else 3)
        )

    def fwd_arrival(c, part):
        landed = kvb.at[y_of(2), c, pair_of(part)]
        return remote(
            landed, landed, f_s.at[c, part], f_r.at[c, part], y_peer(3 if part == 0 else 1)
        )

    def nt(q, kv):
        return lax.dot_general(q, kv, (((1,), (1,)), ((), ())), preferred_element_type=F32)

    def lanes_of(s):
        return [s[:, i : i + hd] for i in range(0, s.shape[1], hd)]

    def fold(parts, op):
        while len(parts) > 1:
            parts = [
                op(parts[i], parts[i + 1]) if i + 1 < len(parts) else parts[i]
                for i in range(0, len(parts), 2)
            ]
        return parts[0]

    def query(cq, j):
        return rowb[:, cq, :, j * hd : (j + 1) * hd].reshape(tile, hd)

    def text_piece(t):
        def piece(q, j):
            span = slice(2 * t, 2 * t + 2)
            nkey = 8 * trow
            kt = textb[span, :, :, j * hd : (j + 1) * hd].reshape(nkey, hd)
            sc = nt(q, kt)
            sc = jnp.where(
                lax.broadcasted_iota(jnp.int32, sc.shape, 1) + t * nkey < tlen_ref[xl], sc, NEG
            )

            def weigh(e):
                vt = textb[span, :, :, tw + j * hd : tw + (j + 1) * hd].reshape(nkey, hd)
                return jnp.dot(e.astype(BF), vt, preferred_element_type=F32)

            return sc, weigh

        return piece

    def own_piece(ck):
        def piece(q, j):
            same = (
                lax.broadcasted_iota(jnp.int32, (tile, tile), 0) // cr_rows
                == lax.broadcasted_iota(jnp.int32, (tile, tile), 1) // cr_rows
            )
            kc = rowb[:, ck, :, tw + j * hd : tw + (j + 1) * hd].reshape(tile, hd)
            kf = fresh[:, ck, :, j * hd : (j + 1) * hd].reshape(tile, hd)
            sc = jnp.where(same, nt(q, kf), nt(q, kc))

            def weigh(e):
                vc = rowb[:, ck, :, 2 * tw + j * hd : 2 * tw + (j + 1) * hd].reshape(tile, hd)
                vf = fresh[:, ck, :, tw + j * hd : tw + (j + 1) * hd].reshape(tile, hd)
                return jnp.dot(
                    jnp.where(same, 0.0, e).astype(BF), vc, preferred_element_type=F32
                ) + jnp.dot(jnp.where(same, e, 0.0).astype(BF), vf, preferred_element_type=F32)

            return sc, weigh

        return piece

    def far_piece(ck, d):
        yy = y_of(d)

        def piece(q, j):
            kc = kvb[yy, ck, :, :, j * hd : (j + 1) * hd].reshape(tile, hd)

            def weigh(e):
                vc = kvb[yy, ck, :, :, tw + j * hd : tw + (j + 1) * hd].reshape(tile, hd)
                return jnp.dot(e.astype(BF), vc, preferred_element_type=F32)

            return nt(q, kc), weigh

        return piece

    def unit(lo, hi, pieces, first=False, then=None):
        def step(cq, carry):
            for j in range(TRI):
                q = query(cq, j)
                got = [p(q, j) for p in pieces]
                top = fold([t for sc, _ in got for t in lanes_of(sc)], jnp.maximum)
                top = jnp.broadcast_to(jnp.max(top, axis=-1, keepdims=True), (tile, hd))
                if not first:
                    old = mst[cq, j]
                    top = jnp.maximum(top, old)
                ref = top * cexp
                sums, av = [], None
                for sc, weigh in got:
                    e = [jnp.exp2(t * cexp - ref) for t in lanes_of(sc)]
                    sums += e
                    add = weigh(jnp.concatenate(e, axis=1))
                    av = add if av is None else av + add
                tot = fold(sums, jnp.add)
                if not first:
                    shrink = jnp.exp2(old * cexp - ref)
                    tot = tot + lst[cq, j] * shrink
                    av = av + acc[cq, j] * shrink
                if then is None:
                    mst[cq, j] = top
                    lst[cq, j] = tot
                    acc[cq, j] = av
                else:
                    then(cq, j, tot, av)
            if then is not None:
                then(cq, None, None, None)
            return carry

        lax.fori_loop(lo, hi, step, 0)

    text = [text_piece(0), text_piece(1)]

    def near(*cks):
        return [far_piece(ck, d) for ck in cks for d in (3, 1)]

    def opp(*cks):
        return [far_piece(ck, 2) for ck in cks]

    lane = lax.broadcasted_iota(jnp.int32, (cr_rows, hd), 1) % (hd // 2)
    col = lax.broadcasted_iota(jnp.int32, (cr_rows, hd), 0).astype(F32)
    freq = freq_ref[...]
    first_pairs = hd // 16
    axis_pairs = (hd // 2 - first_pairs) // 2
    is_row = lane < first_pairs + axis_pairs
    low = lax.broadcasted_iota(jnp.int32, (cr_rows, hd), 1) < hd // 2

    def qkv_step(c, carry):
        for kind in (1, 2, 3):
            img_arrival(c, kind).wait_recv()
            pass_on(c, kind).start()
        img_arrival(c, 0).wait_recv()
        for kind in (1, 2, 3):
            pass_arrival(c, kind).wait_recv()
        rows = rows_of(c)
        for m in range(4):
            a = xf[0, m, rows, :].astype(F32)
            d = xf[1, m, rows, :].astype(F32)
            total = jnp.sum(a, axis=-1, keepdims=True) + jnp.sum(d, axis=-1, keepdims=True)
            mean = total / width
            a = a - mean
            d = d - mean
            var = (
                jnp.sum(a * a, axis=-1, keepdims=True) + jnp.sum(d * d, axis=-1, keepdims=True)
            ) / width
            inv = lax.rsqrt(var + EPS)
            for i, v in enumerate((a, d)):
                scale = 1.0 + mod_ref[1, pl.ds(xl, 1), i * half : (i + 1) * half]
                shift = mod_ref[0, pl.ds(xl, 1), i * half : (i + 1) * half]
                xm[m * cr_rows : (m + 1) * cr_rows, i * half : (i + 1) * half] = (
                    v * inv * scale + shift
                ).astype(BF)
        cosv, sinv = [], []
        for m in range(4):
            row_pos = (patch_ref[y * 4 + m] * NC + c).astype(F32)
            angle = jnp.where(is_row, row_pos, col) * freq
            cosv.append(jnp.cos(angle))
            sine = jnp.sin(angle)
            sinv.append(jnp.where(low, -sine, sine))
        cosv = jnp.concatenate(cosv, axis=0)
        sinv = jnp.concatenate(sinv, axis=0)
        for kind in range(3):
            proj = jnp.dot(
                xm[...], w[:, kind * tw : (kind + 1) * tw], preferred_element_type=F32
            )
            for j in range(TRI):
                t = proj[:, j * hd : (j + 1) * hd]
                if kind < 2:
                    gain = (qg_ref if kind == 0 else kg_ref)[...]
                    ms = jnp.mean(t * t, axis=-1, keepdims=True)
                    t = t * lax.rsqrt(ms + EPS) * gain
                    t = t * cosv + pltpu.roll(t, hd // 2, 1) * sinv
                t = t.astype(BF)
                at = kind * tw + j * hd
                for m in range(4):
                    piece = t[m * cr_rows : (m + 1) * cr_rows]
                    if kind == 0:
                        rowb[m, c, :, at : at + hd] = piece
                    else:
                        fresh[m, c, :, at - tw : at - tw + hd] = piece
        for rel in (1, 2, 3):
            for part in range(2):
                stale_arrival(c, rel, part).wait_recv()
        for m in range(4):
            rowb[m, c, :, tw : 3 * tw] = jnp.where(
                refresh_ref[y * 4 + m] == 1, fresh[m, c], stb[m, rows, :]
            )
        for part, way in ((0, 0), (1, 1), (1, 0), (0, 1)):
            y_send(c, part, way).start()

        @pl.when(c >= 1)
        def _():
            y_arrival(c - 1, 0, 0).wait_recv()
            fwd(c - 1, 0).start()
            y_arrival(c - 1, 1, 1).wait_recv()
            fwd(c - 1, 1).start()
            y_arrival(c - 1, 1, 0).wait_recv()
            y_arrival(c - 1, 0, 1).wait_recv()

        @pl.when(c == 1)
        def _():
            for d in (1, 2, 3):
                ty_arrival(d).wait_recv()
            unit(0, 2, text + [own_piece(0), own_piece(1)], first=True)

        @pl.when(c == 2)
        def _():
            unit(0, 2, near(0, 1))

        return carry

    lax.fori_loop(0, NC, qkv_step, 0)

    w_first.wait_recv()
    for i in range(len(zpeers)):
        w_pass(i).start()

    def opp_wait(c):
        fwd_arrival(c, 0).wait_recv()
        fwd_arrival(c, 1).wait_recv()

    unit(2, 4, text + [own_piece(ck) for ck in range(NC)], first=True)
    opp_wait(0)
    opp_wait(1)
    unit(0, 2, [own_piece(2), own_piece(3)] + opp(0, 1))
    y_arrival(NC - 1, 0, 0).wait_recv()
    fwd(NC - 1, 0).start()
    y_arrival(NC - 1, 1, 1).wait_recv()
    fwd(NC - 1, 1).start()
    unit(2, 4, near(0, 1) + opp(0, 1))
    y_arrival(NC - 1, 1, 0).wait_recv()
    y_arrival(NC - 1, 0, 1).wait_recv()
    unit(0, 4, near(2, 3))
    opp_wait(2)
    opp_wait(3)

    def att_slot(hh, m, c):
        at = pl.multiple_of((c % 2) * cr_rows, cr_rows)
        return att.at[hh, m % 2, c // 2, m // 2, pl.ds(at, cr_rows)]

    def a_send(c, rel, other):
        i = rel * 2 + other
        return remote(
            osend.at[member(rel), c],
            att_slot(h, mine, c),
            a_s.at[c, i],
            a_r.at[c, i],
            row_peer(rel, other),
        )

    def a_arrival(c, rel, other):
        i = rel * 2 + other
        d = att_slot((h + other) % 2, member(rel), c)
        return remote(d, d, a_s.at[c, i], a_r.at[c, i], row_peer(rel, other))

    far_order = ((2, 1), (0, 1), (3, 1), (1, 1), (2, 0), (3, 0), (1, 0))

    def deliver(cq, j, tot, av):
        if j is not None:
            o = (av / jnp.sum(tot, axis=-1, keepdims=True)).astype(BF)
            for m in range(4):
                osend[m, cq, :, j * hd : (j + 1) * hd] = o[m * cr_rows : (m + 1) * cr_rows]
            return
        for rel, other in far_order:
            a_send(cq, rel, other).start()
        at = pl.multiple_of((cq % 2) * cr_rows, cr_rows)
        att[h, k, cq // 2, xl, pl.ds(at, cr_rows)] = osend[mine, cq]

    unit(0, 4, opp(2, 3), then=deliver)

    for c_ in late:
        c_.wait()
    for i, (db, dk, dev) in enumerate(zpeers):
        rows = w_rows(w_slot(db, dk))
        remote(woth.at[rows], woth.at[rows], w_s.at[1 + i], w_r.at[1 + i], dev).wait_recv()

    def out_copy(s, p):
        rows = pl.ds(pl.multiple_of(s * 2 * cr_rows, cr_rows), 2 * cr_rows)
        return pltpu.make_async_copy(outv.at[p, rows], out_hbm.at[p, rows], lsem.at[11 + 2 * s + p])

    def finish(s, carry):
        for rel, other in far_order[::-1]:
            for e in range(2):
                a_arrival(2 * s + e, rel, other).wait_recv()
        proj = None
        for i, wref in enumerate((wown, woth)):
            hh = (h + i) % 2
            for kk in range(2):
                lhs = att[hh, kk, s].reshape(tile, tw)
                part = jnp.dot(
                    lhs, wref[kk * tw : (kk + 1) * tw, :], preferred_element_type=F32
                )
                proj = part if proj is None else proj + part
        rows = pl.ds(pl.multiple_of(s * 2 * cr_rows, cr_rows), 2 * cr_rows)
        for p in range(2):
            gate = mod_ref[2, pl.ds(p, 1), pl.ds(own_off, half)]
            outv[p, rows, :] = (
                xo[p, rows, :].astype(F32)
                + gate * proj[p * 2 * cr_rows : (p + 1) * 2 * cr_rows]
                + cr[p, rows, :].astype(F32)
            ).astype(BF)
            out_copy(s, p).start()
        return carry

    lax.fori_loop(0, 2, finish, 0)

    for s in range(2):
        for p in range(2):
            out_copy(s, p).wait()

    def drain(c, carry):
        for kind in range(4):
            img(c, kind).wait_send()
        for kind in (1, 2, 3):
            pass_on(c, kind).wait_send()
        for rel in (1, 2, 3):
            for part in range(2):
                stale(c, rel, part).wait_send()
        for part in range(2):
            for way in range(2):
                y_send(c, part, way).wait_send()
            fwd(c, part).wait_send()
        for rel, other in far_order:
            a_send(c, rel, other).wait_send()
        return carry

    lax.fori_loop(0, NC, drain, 0)
    for rel in (1, 2, 3):
        for part in range(2):
            txt(rel, part).wait_send()
    for d in (1, 2, 3):
        ty(d).wait_send()
    w_first.wait_send()
    for i in range(len(zpeers)):
        w_pass(i).wait_send()


def per_device(
    nb,
    image_hidden,
    modulation,
    qkv_weight,
    out_weight,
    q_gain,
    k_gain,
    text_keys,
    text_values,
    stale_keys,
    stale_values,
    cached_residual,
    patch_of,
    refresh,
    text_len,
):
    prompts, rows, half = image_hidden.shape
    hd = q_gain.shape[0]
    channels = out_weight.shape[0]
    tw = TRI * hd
    cr_rows = rows // NC
    trow = text_keys.shape[1]
    smem = pl.BlockSpec(memory_space=pltpu.SMEM)
    vmem = pl.BlockSpec(memory_space=pltpu.VMEM)
    hbm = pl.BlockSpec(memory_space=pl.ANY)
    dma = pltpu.SemaphoreType.DMA
    ns = 2 * nb
    return pl.pallas_call(
        functools.partial(kernel, nb),
        name="joint",
        out_shape=jax.ShapeDtypeStruct(image_hidden.shape, BF),
        in_specs=[smem] * 3 + [vmem] * 4 + [hbm] * 8,
        out_specs=hbm,
        scratch_shapes=[
            pltpu.VMEM((2 * half, 3 * tw), BF),
            pltpu.VMEM((2, 4, rows, half), BF),
            pltpu.VMEM((prompts, rows, half), BF),
            pltpu.VMEM((prompts, rows, half), BF),
            pltpu.VMEM((4 * cr_rows, 2 * half), BF),
            pltpu.VMEM((4, rows, 2 * tw), BF),
            pltpu.VMEM((4, NC, cr_rows, 2 * tw), BF),
            pltpu.VMEM((4, NC, cr_rows, 3 * tw), BF),
            pltpu.VMEM((4, NC, 4, cr_rows, 2 * tw), BF),
            pltpu.VMEM((4, 4, trow, 2 * tw), BF),
            pltpu.VMEM((NC, TRI, 4 * cr_rows, hd), F32),
            pltpu.VMEM((NC, TRI, 4 * cr_rows, hd), F32),
            pltpu.VMEM((NC, TRI, 4 * cr_rows, hd), F32),
            pltpu.VMEM((4, NC, cr_rows, tw), BF),
            pltpu.VMEM((2, 2, 2, 2, 2 * cr_rows, tw), BF),
            pltpu.VMEM((channels, half), BF),
            pltpu.VMEM((channels, half), BF),
            pltpu.VMEM((prompts, rows, half), BF),
            dma((15,)),
            dma((NC, 4)),
            dma((NC, 4)),
            dma((NC, 3)),
            dma((NC, 3)),
            dma((NC, 4, 2)),
            dma((NC, 4, 2)),
            dma((4, 2)),
            dma((4, 2)),
            dma((3,)),
            dma((3,)),
            dma((NC, 2, 2)),
            dma((NC, 2, 2)),
            dma((NC, 2)),
            dma((NC, 2)),
            dma((NC, 8)),
            dma((NC, 8)),
            dma((ns,)),
            dma((ns,)),
        ],
        compiler_params=pltpu.CompilerParams(
            collective_id=0, has_side_effects=True, vmem_limit_bytes=66 * 1024 * 1024 - 2097152
        ),
    )(
        patch_of,
        refresh,
        text_len,
        jnp.transpose(modulation, (1, 0, 2)),
        pair_frequency(hd),
        q_gain.reshape(1, hd),
        k_gain.reshape(1, hd),
        image_hidden,
        jnp.transpose(qkv_weight, (1, 0, 2)),
        out_weight,
        text_keys,
        text_values,
        stale_keys,
        stale_values,
        cached_residual,
    )


def solution(mesh):
    in_specs = (
        P("batch", "seq", "head"),
        P("batch", None, None),
        P(None, None, "head"),
        P("head", None),
        P(),
        P(),
        P("batch", "seq", "head"),
        P("batch", "seq", "head"),
        P("batch", "seq", "head"),
        P("batch", "seq", "head"),
        P("batch", "seq", "head"),
        P("batch"),
        P("batch"),
        P("batch"),
    )
    out_specs = P("batch", "seq", "head")
    return jax.shard_map(
        functools.partial(per_device, mesh.shape["batch"]),
        mesh=mesh,
        in_specs=in_specs,
        out_specs=out_specs,
        check_vma=False,
    )
```

```python
import functools
import math

import jax
import jax.numpy as jnp
import numpy as np
from jax import lax
from jax.experimental import pallas as pl
from jax.experimental.pallas import tpu as pltpu
from jax.sharding import PartitionSpec as P

GRID_W = 64
EPS = 1e-06
NEG = -1e30
MESH = pl.DeviceIdType.MESH
BF = jnp.bfloat16
F32 = jnp.float32

NC = 8
NT = 4
TRI = 3


def pair_frequency(head_dim):
    half_dim = head_dim // 2
    first_pairs = head_dim // 16
    axis_pairs = (half_dim - first_pairs) // 2
    pair = np.arange(half_dim)
    local = np.where(pair < first_pairs + axis_pairs, pair - first_pairs, pair - first_pairs - axis_pairs)
    exponent = -local.astype(np.float32) / np.float32(axis_pairs)
    power = np.power(10000.0, exponent.astype(np.float64))
    frequency = np.where(pair < first_pairs, 0.0, power).astype(np.float32)
    return np.concatenate([frequency, frequency]).reshape(1, head_dim)


def kernel(
    nb,
    patch_ref,
    refresh_ref,
    tlen_ref,
    mod_ref,
    freq_ref,
    qg_ref,
    kg_ref,
    x_hbm,
    w_hbm,
    wo_hbm,
    tk_hbm,
    tv_hbm,
    sk_hbm,
    sv_hbm,
    cr_hbm,
    out_hbm,
    w,
    xf,
    xo,
    cr,
    xm,
    stb,
    fresh,
    rowb,
    kvb,
    textb,
    acc,
    mst,
    lst,
    osend,
    att,
    wown,
    woth,
    outv,
    lsem,
    img_s,
    img_r,
    sib_s,
    sib_r,
    st_s,
    st_r,
    txt_s,
    txt_r,
    ty_s,
    ty_r,
    y_s,
    y_r,
    f_s,
    f_r,
    a_s,
    a_r,
    w_s,
    w_r,
):
    b = lax.axis_index("batch")
    me = lax.axis_index("seq")
    h = lax.axis_index("head")
    k = me % 2
    xl = (me // 2) % 2
    y = me // 4
    mine = me % 4
    half = xo.shape[2]
    width = 2 * half
    cr_rows = xo.shape[1] // NC
    t_rows = xo.shape[1] // NT
    tile = 4 * t_rows
    hd = 128
    tw = TRI * hd
    ns = 2 * nb
    wrows = woth.shape[0] // ns
    trow = tk_hbm.shape[1]
    cexp = (hd ** -0.5) * math.log2(math.e)

    def member(rel):
        return ((xl + rel // 2) % 2) * 2 + (k + rel % 2) % 2

    def row_peer(rel, other=0):
        return {"seq": y * 4 + member(rel), "head": (h + other) % 2}

    def y_of(d):
        return (y + d) % 4

    def y_peer(d):
        return {"seq": y_of(d) * 4 + mine}

    def remote(src, dst, ss, rs, dev):
        return pltpu.make_async_remote_copy(src, dst, ss, rs, device_id=dev, device_id_type=MESH)

    def rows_of(c):
        return pl.ds(pl.multiple_of(c * cr_rows, cr_rows), cr_rows)

    def tri_cols(kk):
        return pl.ds(pl.multiple_of(kk * tw, 128), tw)

    own_off = pl.multiple_of(h * half, 128)
    part_off = pl.multiple_of((1 - h) * half, 128)

    local = [
        pltpu.make_async_copy(x_hbm.at[xl], xf.at[h, mine], lsem.at[0]),
        pltpu.make_async_copy(sk_hbm.at[xl, :, tri_cols(k)], stb.at[mine, :, 0:tw], lsem.at[1]),
        pltpu.make_async_copy(
            sv_hbm.at[xl, :, tri_cols(k)], stb.at[mine, :, tw : 2 * tw], lsem.at[2]
        ),
        pltpu.make_async_copy(
            tk_hbm.at[xl, :, tri_cols(k)], textb.at[y, mine, :, 0:tw], lsem.at[3]
        ),
        pltpu.make_async_copy(
            tv_hbm.at[xl, :, tri_cols(k)], textb.at[y, mine, :, tw : 2 * tw], lsem.at[4]
        ),
    ]
    for kind in range(3):
        local.append(
            pltpu.make_async_copy(
                w_hbm.at[kind, :, tri_cols(k)], w.at[:, kind * tw : (kind + 1) * tw], lsem.at[5 + kind]
            )
        )
    late = [
        pltpu.make_async_copy(wo_hbm.at[:, pl.ds(own_off, half)], wown, lsem.at[8]),
        pltpu.make_async_copy(cr_hbm, cr, lsem.at[9]),
        pltpu.make_async_copy(x_hbm, xo, lsem.at[10]),
    ]
    for c_ in local:
        c_.start()

    peers = [y_peer(d) for d in (2, 1, 3)]
    peers += [row_peer(r, 1) for r in range(4)]
    zpeers = []
    for db in range(nb):
        for dk in range(2):
            if db == 0 and dk == 0:
                continue
            dev = {"batch": (b + db) % nb, "seq": me + dk * (1 - 2 * k)}
            zpeers.append((db, dk, dev))
            if db != 0:
                peers.append(dev)
    peers += [row_peer(r) for r in (1, 2, 3)]
    bar = pltpu.get_barrier_semaphore()
    for p_ in peers:
        pl.semaphore_signal(bar, inc=1, device_id=p_, device_id_type=MESH)
    pl.semaphore_wait(bar, len(peers))

    def txt(rel, part):
        m = member(rel)
        return remote(
            (tk_hbm if part == 0 else tv_hbm).at[m // 2, :, tri_cols(m % 2)],
            textb.at[y, mine, :, part * tw : (part + 1) * tw],
            txt_s.at[rel],
            txt_r.at[rel],
            row_peer(rel),
        )

    def txt_arrival(rel):
        landed = textb.at[y, member(rel)]
        return remote(landed, landed, txt_s.at[rel], txt_r.at[rel], row_peer(rel))

    def img_peer(kind):
        return row_peer((1, 0, 2, 2)[kind], (0, 1, 0, 1)[kind])

    def img(c, kind):
        p = xl if kind < 2 else 1 - xl
        return remote(
            x_hbm.at[p, rows_of(c)],
            xf.at[h, mine, rows_of(c)],
            img_s.at[kind],
            img_r.at[c, kind],
            img_peer(kind),
        )

    def img_landed(c, kind):
        m = member((1, 0, 2, 2)[kind])
        return xf.at[(h + (0, 1, 0, 1)[kind]) % 2, m, rows_of(c)]

    def img_arrival(c, kind):
        d = img_landed(c, kind)
        return remote(d, d, img_s.at[kind], img_r.at[c, kind], img_peer(kind))

    def pass_on(c, kind):
        d = img_landed(c, kind)
        return remote(d, d, sib_s.at[kind - 1], sib_r.at[c, kind - 1], row_peer(1))

    def pass_arrival(c, kind):
        m = member((1, 1, 3, 3)[kind])
        d = xf.at[(h + (0, 1, 0, 1)[kind]) % 2, m, rows_of(c)]
        return remote(d, d, sib_s.at[kind - 1], sib_r.at[c, kind - 1], row_peer(1))

    def stale(c, rel, part):
        m = member(rel)
        return remote(
            (sk_hbm if part == 0 else sv_hbm).at[m // 2, rows_of(c), tri_cols(m % 2)],
            stb.at[mine, rows_of(c), part * tw : (part + 1) * tw],
            st_s.at[rel],
            st_r.at[c, rel],
            row_peer(rel),
        )

    def stale_arrival(c, rel):
        d = stb.at[member(rel), rows_of(c)]
        return remote(d, d, st_s.at[rel], st_r.at[c, rel], row_peer(rel))

    def send_image(c):
        for kind in (1, 2, 3, 0):
            img(c, kind).start()

    def send_stale(c):
        for rel in (2, 3, 1):
            for part in range(2):
                stale(c, rel, part).start()

    for rel in (2, 3, 1):
        for part in range(2):
            txt(rel, part).start()

    def send_chunk(c, carry):
        send_image(c)
        send_stale(c)
        return carry

    lax.fori_loop(0, NC, send_chunk, 0)

    def w_slot(db, dk):
        return ((b + nb - db) % nb) * 2 + (k + dk) % 2

    def w_rows(s):
        return pl.ds(pl.multiple_of(s * wrows, wrows), wrows)

    my_rows = w_rows(b * 2 + k)

    def w_pass(i):
        return remote(
            woth.at[my_rows], woth.at[my_rows], w_s.at[1 + i], w_r.at[1 + i], zpeers[i][2]
        )

    w_first = remote(
        wo_hbm.at[my_rows, pl.ds(part_off, half)],
        woth.at[my_rows],
        w_s.at[0],
        w_r.at[0],
        row_peer(2, 1),
    )
    w_first.start()
    for c_ in late:
        c_.start()

    def ty(d):
        return remote(textb.at[y], textb.at[y], ty_s.at[d - 1], ty_r.at[d - 1], y_peer(d))

    def ty_arrival(d):
        landed = textb.at[y_of(4 - d)]
        return remote(landed, landed, ty_s.at[d - 1], ty_r.at[d - 1], y_peer(4 - d))

    for c_ in local:
        c_.wait()
    for rel in (1, 2, 3):
        txt_arrival(rel).wait_recv()
    for d in (1, 3, 2):
        ty(d).start()

    def pair_of(part):
        return pl.ds(2 * ((xl + part) % 2), 2)

    def y_send(c, part, way):
        return remote(
            rowb.at[pair_of(part), rows_of(c), tw : 3 * tw],
            kvb.at[y, pair_of(part), rows_of(c)],
            y_s.at[part, way],
            y_r.at[c, part, way],
            y_peer(1 if way == 0 else 3),
        )

    def y_arrival(c, part, way):
        d = 3 if way == 0 else 1
        landed = kvb.at[y_of(d), pair_of(part), rows_of(c)]
        return remote(landed, landed, y_s.at[part, way], y_r.at[c, part, way], y_peer(d))

    def fwd(c, part):
        held = kvb.at[y_of(3 if part == 0 else 1), pair_of(part), rows_of(c)]
        return remote(
            held, held, f_s.at[part], f_r.at[c, part], y_peer(1 if part == 0 else 3)
        )

    def fwd_arrival(c, part):
        landed = kvb.at[y_of(2), pair_of(part), rows_of(c)]
        return remote(
            landed, landed, f_s.at[part], f_r.at[c, part], y_peer(3 if part == 0 else 1)
        )

    def nt(q, kv):
        return lax.dot_general(q, kv, (((1,), (1,)), ((), ())), preferred_element_type=F32)

    def lanes_of(s):
        return [s[:, i : i + hd] for i in range(0, s.shape[1], hd)]

    def fold(parts, op):
        while len(parts) > 1:
            parts = [
                op(parts[i], parts[i + 1]) if i + 1 < len(parts) else parts[i]
                for i in range(0, len(parts), 2)
            ]
        return parts[0]

    def tile_rows(c):
        return pl.ds(pl.multiple_of(c * t_rows, t_rows), t_rows)

    def query(cq, j):
        return rowb[:, tile_rows(cq), j * hd : (j + 1) * hd].reshape(tile, hd)

    def text_piece(t):
        def piece(q, j):
            span = slice(2 * t, 2 * t + 2)
            nkey = 8 * trow
            kt = textb[span, :, :, j * hd : (j + 1) * hd].reshape(nkey, hd)
            sc = nt(q, kt)
            sc = jnp.where(
                lax.broadcasted_iota(jnp.int32, sc.shape, 1) + t * nkey < tlen_ref[xl], sc, NEG
            )

            def weigh(e):
                vt = textb[span, :, :, tw + j * hd : tw + (j + 1) * hd].reshape(nkey, hd)
                return jnp.dot(e.astype(BF), vt, preferred_element_type=F32)

            return sc, weigh

        return piece

    def own_piece(ck):
        def piece(q, j):
            same = (
                lax.broadcasted_iota(jnp.int32, (tile, tile), 0) // t_rows
                == lax.broadcasted_iota(jnp.int32, (tile, tile), 1) // t_rows
            )
            kc = rowb[:, tile_rows(ck), tw + j * hd : tw + (j + 1) * hd].reshape(tile, hd)
            kf = fresh[:, tile_rows(ck), j * hd : (j + 1) * hd].reshape(tile, hd)
            sc = jnp.where(same, nt(q, kf), nt(q, kc))

            def weigh(e):
                vc = rowb[:, tile_rows(ck), 2 * tw + j * hd : 2 * tw + (j + 1) * hd].reshape(tile, hd)
                vf = fresh[:, tile_rows(ck), tw + j * hd : tw + (j + 1) * hd].reshape(tile, hd)
                return jnp.dot(
                    jnp.where(same, 0.0, e).astype(BF), vc, preferred_element_type=F32
                ) + jnp.dot(jnp.where(same, e, 0.0).astype(BF), vf, preferred_element_type=F32)

            return sc, weigh

        return piece

    def far_piece(ck, d):
        yy = y_of(d)

        def piece(q, j):
            kc = kvb[yy, :, tile_rows(ck), j * hd : (j + 1) * hd].reshape(tile, hd)

            def weigh(e):
                vc = kvb[yy, :, tile_rows(ck), tw + j * hd : tw + (j + 1) * hd].reshape(tile, hd)
                return jnp.dot(e.astype(BF), vc, preferred_element_type=F32)

            return nt(q, kc), weigh

        return piece

    def unit(lo, hi, pieces, first=False, then=None):
        def step(cq, carry):
            for j in range(TRI):
                q = query(cq, j)
                got = [p(q, j) for p in pieces]
                top = fold([t for sc, _ in got for t in lanes_of(sc)], jnp.maximum)
                top = jnp.broadcast_to(jnp.max(top, axis=-1, keepdims=True), (tile, hd))
                if not first:
                    old = mst[cq, j]
                    top = jnp.maximum(top, old)
                ref = top * cexp
                sums, av = [], None
                for sc, weigh in got:
                    e = [jnp.exp2(t * cexp - ref) for t in lanes_of(sc)]
                    sums += e
                    add = weigh(jnp.concatenate(e, axis=1))
                    av = add if av is None else av + add
                tot = fold(sums, jnp.add)
                if not first:
                    shrink = jnp.exp2(old * cexp - ref)
                    tot = tot + lst[cq, j] * shrink
                    av = av + acc[cq, j] * shrink
                if then is None:
                    mst[cq, j] = top
                    lst[cq, j] = tot
                    acc[cq, j] = av
                else:
                    then(cq, j, tot, av)
            if then is not None:
                then(cq, None, None, None)
            return carry

        lax.fori_loop(lo, hi, step, 0)

    text = [text_piece(0), text_piece(1)]

    def near(*cks):
        return [far_piece(ck, d) for ck in cks for d in (3, 1)]

    def opp(*cks):
        return [far_piece(ck, 2) for ck in cks]

    def own(*cks):
        return [own_piece(ck) for ck in cks]

    def opp_wait(c):
        fwd_arrival(c, 0).wait_recv()
        fwd_arrival(c, 1).wait_recv()

    lane = lax.broadcasted_iota(jnp.int32, (cr_rows, hd), 1) % (hd // 2)
    col = lax.broadcasted_iota(jnp.int32, (cr_rows, hd), 0).astype(F32)
    freq = freq_ref[...]
    first_pairs = hd // 16
    axis_pairs = (hd // 2 - first_pairs) // 2
    is_row = lane < first_pairs + axis_pairs
    low = lax.broadcasted_iota(jnp.int32, (cr_rows, hd), 1) < hd // 2

    def qkv_step(c, carry):
        for kind in (1, 2, 3):
            img_arrival(c, kind).wait_recv()
            pass_on(c, kind).start()
        img_arrival(c, 0).wait_recv()
        for kind in (1, 2, 3):
            pass_arrival(c, kind).wait_recv()
        rows = rows_of(c)
        for m in range(4):
            a = xf[0, m, rows, :].astype(F32)
            d = xf[1, m, rows, :].astype(F32)
            total = jnp.sum(a, axis=-1, keepdims=True) + jnp.sum(d, axis=-1, keepdims=True)
            mean = total / width
            a = a - mean
            d = d - mean
            var = (
                jnp.sum(a * a, axis=-1, keepdims=True) + jnp.sum(d * d, axis=-1, keepdims=True)
            ) / width
            inv = lax.rsqrt(var + EPS)
            for i, v in enumerate((a, d)):
                scale = 1.0 + mod_ref[1, pl.ds(xl, 1), i * half : (i + 1) * half]
                shift = mod_ref[0, pl.ds(xl, 1), i * half : (i + 1) * half]
                xm[m * cr_rows : (m + 1) * cr_rows, i * half : (i + 1) * half] = (
                    v * inv * scale + shift
                ).astype(BF)
        cosv, sinv = [], []
        for m in range(4):
            raster = patch_ref[y * 4 + m] * (NC * cr_rows) + c * cr_rows
            row_pos = (raster // GRID_W).astype(F32)
            col_pos = (raster % GRID_W).astype(F32) + col
            angle = jnp.where(is_row, row_pos, col_pos) * freq
            cosv.append(jnp.cos(angle))
            sine = jnp.sin(angle)
            sinv.append(jnp.where(low, -sine, sine))
        cosv = jnp.concatenate(cosv, axis=0)
        sinv = jnp.concatenate(sinv, axis=0)
        for kind in range(3):
            proj = jnp.dot(
                xm[...], w[:, kind * tw : (kind + 1) * tw], preferred_element_type=F32
            )
            for j in range(TRI):
                t = proj[:, j * hd : (j + 1) * hd]
                if kind < 2:
                    gain = (qg_ref if kind == 0 else kg_ref)[...]
                    ms = jnp.mean(t * t, axis=-1, keepdims=True)
                    t = t * lax.rsqrt(ms + EPS) * gain
                    t = t * cosv + pltpu.roll(t, hd // 2, 1) * sinv
                t = t.astype(BF)
                at = kind * tw + j * hd
                for m in range(4):
                    piece = t[m * cr_rows : (m + 1) * cr_rows]
                    if kind == 0:
                        rowb[m, rows, at : at + hd] = piece
                    else:
                        fresh[m, rows, at - tw : at - tw + hd] = piece
        for rel in (1, 2, 3):
            stale_arrival(c, rel).wait_recv()
        for m in range(4):
            rowb[m, rows, tw : 3 * tw] = jnp.where(
                refresh_ref[y * 4 + m] == 1, fresh[m, rows, :], stb[m, rows, :]
            )
        for part, way in ((0, 0), (1, 1), (1, 0), (0, 1)):
            y_send(c, part, way).start()

        @pl.when(c >= 1)
        def _():
            y_arrival(c - 1, 0, 0).wait_recv()
            fwd(c - 1, 0).start()
            y_arrival(c - 1, 1, 1).wait_recv()
            fwd(c - 1, 1).start()
            y_arrival(c - 1, 1, 0).wait_recv()
            y_arrival(c - 1, 0, 1).wait_recv()

        @pl.when(c == 3)
        def _():
            for d in (1, 2, 3):
                ty_arrival(d).wait_recv()
            unit(0, 2, text + own(0, 1), first=True)

        @pl.when(c == 4)
        def _():
            unit(0, 2, near(0, 1))

        @pl.when(c == 5)
        def _():
            unit(2, 3, text + own(0, 1, 2), first=True)

        @pl.when(c == 6)
        def _():
            w_first.wait_recv()
            for i in range(len(zpeers)):
                w_pass(i).start()
            for e in range(4):
                opp_wait(e)
            unit(0, 2, own(2) + opp(0, 1))

        return carry

    lax.fori_loop(0, NC, qkv_step, 0)

    unit(2, 3, own(3) + near(0, 1) + opp(0, 1))
    unit(0, 2, own(3) + near(2))
    y_arrival(NC - 1, 0, 0).wait_recv()
    fwd(NC - 1, 0).start()
    y_arrival(NC - 1, 1, 1).wait_recv()
    fwd(NC - 1, 1).start()
    y_arrival(NC - 1, 1, 0).wait_recv()
    y_arrival(NC - 1, 0, 1).wait_recv()
    unit(0, 2, near(3))
    unit(3, 4, text + own(0, 1, 2, 3), first=True)
    for e in range(4, NC):
        opp_wait(e)

    def att_slot(hh, m, c):
        at = pl.multiple_of((c % 2) * t_rows, t_rows)
        return att.at[hh, m % 2, c // 2, m // 2, pl.ds(at, t_rows)]

    def a_send(c, rel, other):
        i = rel * 2 + other
        return remote(
            osend.at[member(rel), c],
            att_slot(h, mine, c),
            a_s.at[i],
            a_r.at[c, i],
            row_peer(rel, other),
        )

    def a_arrival(c, rel, other):
        i = rel * 2 + other
        d = att_slot((h + other) % 2, member(rel), c)
        return remote(d, d, a_s.at[i], a_r.at[c, i], row_peer(rel, other))

    far_order = ((2, 1), (0, 1), (3, 1), (1, 1), (2, 0), (3, 0), (1, 0))

    def deliver(cq, j, tot, av):
        if j is not None:
            o = (av / jnp.sum(tot, axis=-1, keepdims=True)).astype(BF)
            for m in range(4):
                osend[m, cq, :, j * hd : (j + 1) * hd] = o[m * t_rows : (m + 1) * t_rows]
            return
        for rel, other in far_order:
            a_send(cq, rel, other).start()
        at = pl.multiple_of((cq % 2) * t_rows, t_rows)
        att[h, k, cq // 2, xl, pl.ds(at, t_rows)] = osend[mine, cq]

    unit(0, 2, opp(2, 3), then=deliver)
    unit(2, 3, near(2, 3) + opp(2, 3), then=deliver)
    unit(3, 4, near(0, 1, 2, 3))
    unit(3, 4, opp(0, 1, 2, 3), then=deliver)

    for c_ in late:
        c_.wait()
    for i, (db, dk, dev) in enumerate(zpeers):
        rows = w_rows(w_slot(db, dk))
        remote(woth.at[rows], woth.at[rows], w_s.at[1 + i], w_r.at[1 + i], dev).wait_recv()

    def out_copy(s, p):
        rows = pl.ds(pl.multiple_of(s * 2 * t_rows, t_rows), 2 * t_rows)
        return pltpu.make_async_copy(outv.at[p, rows], out_hbm.at[p, rows], lsem.at[11 + 2 * s + p])

    def finish(s, carry):
        for rel, other in far_order[::-1]:
            for e in range(2):
                a_arrival(2 * s + e, rel, other).wait_recv()
        proj = None
        for i, wref in enumerate((wown, woth)):
            hh = (h + i) % 2
            for kk in range(2):
                lhs = att[hh, kk, s].reshape(tile, tw)
                part = jnp.dot(
                    lhs, wref[kk * tw : (kk + 1) * tw, :], preferred_element_type=F32
                )
                proj = part if proj is None else proj + part
        rows = pl.ds(pl.multiple_of(s * 2 * t_rows, t_rows), 2 * t_rows)
        for p in range(2):
            gate = mod_ref[2, pl.ds(p, 1), pl.ds(own_off, half)]
            outv[p, rows, :] = (
                xo[p, rows, :].astype(F32)
                + gate * proj[p * 2 * t_rows : (p + 1) * 2 * t_rows]
                + cr[p, rows, :].astype(F32)
            ).astype(BF)
            out_copy(s, p).start()
        return carry

    lax.fori_loop(0, 2, finish, 0)

    for s in range(2):
        for p in range(2):
            out_copy(s, p).wait()

    def sent(buf, sem):
        remote(buf, buf, sem, sem, row_peer(1)).wait_send()

    for kind in range(4):
        sent(xf.at[0, 0], img_s.at[kind])
    for kind in range(3):
        sent(xf.at[0, 0], sib_s.at[kind])
    for rel in (1, 2, 3):
        sent(stb.at[0], st_s.at[rel])
        sent(textb.at[0, 0], txt_s.at[rel])
    for part in range(2):
        for way in range(2):
            sent(kvb.at[0, 0:2], y_s.at[part, way])
        sent(kvb.at[0, 0:2], f_s.at[part])
    for rel, other in far_order:
        sent(osend.at[0], a_s.at[rel * 2 + other])
    for d in (1, 2, 3):
        ty(d).wait_send()
    w_first.wait_send()
    for i in range(len(zpeers)):
        w_pass(i).wait_send()


def per_device(
    nb,
    image_hidden,
    modulation,
    qkv_weight,
    out_weight,
    q_gain,
    k_gain,
    text_keys,
    text_values,
    stale_keys,
    stale_values,
    cached_residual,
    patch_of,
    refresh,
    text_len,
):
    prompts, rows, half = image_hidden.shape
    hd = q_gain.shape[0]
    channels = out_weight.shape[0]
    tw = TRI * hd
    cr_rows = rows // NC
    t_rows = rows // NT
    trow = text_keys.shape[1]
    smem = pl.BlockSpec(memory_space=pltpu.SMEM)
    vmem = pl.BlockSpec(memory_space=pltpu.VMEM)
    hbm = pl.BlockSpec(memory_space=pl.ANY)
    dma = pltpu.SemaphoreType.DMA
    ns = 2 * nb
    return pl.pallas_call(
        functools.partial(kernel, nb),
        name="joint",
        out_shape=jax.ShapeDtypeStruct(image_hidden.shape, BF),
        in_specs=[smem] * 3 + [vmem] * 4 + [hbm] * 8,
        out_specs=hbm,
        scratch_shapes=[
            pltpu.VMEM((2 * half, 3 * tw), BF),
            pltpu.VMEM((2, 4, rows, half), BF),
            pltpu.VMEM((prompts, rows, half), BF),
            pltpu.VMEM((prompts, rows, half), BF),
            pltpu.VMEM((4 * cr_rows, 2 * half), BF),
            pltpu.VMEM((4, rows, 2 * tw), BF),
            pltpu.VMEM((4, rows, 2 * tw), BF),
            pltpu.VMEM((4, rows, 3 * tw), BF),
            pltpu.VMEM((4, 4, rows, 2 * tw), BF),
            pltpu.VMEM((4, 4, trow, 2 * tw), BF),
            pltpu.VMEM((NT, TRI, 4 * t_rows, hd), F32),
            pltpu.VMEM((NT, TRI, 4 * t_rows, hd), F32),
            pltpu.VMEM((NT, TRI, 4 * t_rows, hd), F32),
            pltpu.VMEM((4, NT, t_rows, tw), BF),
            pltpu.VMEM((2, 2, 2, 2, 2 * t_rows, tw), BF),
            pltpu.VMEM((channels, half), BF),
            pltpu.VMEM((channels, half), BF),
            pltpu.VMEM((prompts, rows, half), BF),
            dma((15,)),
            dma((4,)),
            dma((NC, 4)),
            dma((3,)),
            dma((NC, 3)),
            dma((4,)),
            dma((NC, 4)),
            dma((4,)),
            dma((4,)),
            dma((3,)),
            dma((3,)),
            dma((2, 2)),
            dma((NC, 2, 2)),
            dma((2,)),
            dma((NC, 2)),
            dma((8,)),
            dma((NT, 8)),
            dma((ns,)),
            dma((ns,)),
        ],
        compiler_params=pltpu.CompilerParams(
            collective_id=0, has_side_effects=True, vmem_limit_bytes=66 * 1024 * 1024 - 2097152
        ),
    )(
        patch_of,
        refresh,
        text_len,
        jnp.transpose(modulation, (1, 0, 2)),
        jnp.asarray(pair_frequency(hd)),
        q_gain.reshape(1, hd),
        k_gain.reshape(1, hd),
        image_hidden,
        jnp.transpose(qkv_weight, (1, 0, 2)),
        out_weight,
        text_keys,
        text_values,
        stale_keys,
        stale_values,
        cached_residual,
    )


def solution(mesh):
    in_specs = (
        P("batch", "seq", "head"),
        P("batch", None, None),
        P(None, None, "head"),
        P("head", None),
        P(),
        P(),
        P("batch", "seq", "head"),
        P("batch", "seq", "head"),
        P("batch", "seq", "head"),
        P("batch", "seq", "head"),
        P("batch", "seq", "head"),
        P("batch"),
        P("batch"),
        P("batch"),
    )
    out_specs = P("batch", "seq", "head")
    return jax.shard_map(
        functools.partial(per_device, mesh.shape["batch"]),
        mesh=mesh,
        in_specs=in_specs,
        out_specs=out_specs,
        check_vma=False,
    )
```

```python
import functools
import math

import jax
import jax.numpy as jnp
import numpy as np
from jax import lax
from jax.experimental import pallas as pl
from jax.experimental.pallas import tpu as pltpu
from jax.sharding import PartitionSpec as P

GRID_W = 64
EPS = 1e-06
NEG = -1e30
MESH = pl.DeviceIdType.MESH
BF = jnp.bfloat16
F32 = jnp.float32

NC = 8
NT = 4
TRI = 3


def pair_frequency(head_dim):
    half_dim = head_dim // 2
    first_pairs = head_dim // 16
    axis_pairs = (half_dim - first_pairs) // 2
    pair = np.arange(half_dim)
    local = np.where(pair < first_pairs + axis_pairs, pair - first_pairs, pair - first_pairs - axis_pairs)
    exponent = -local.astype(np.float32) / np.float32(axis_pairs)
    power = np.power(10000.0, exponent.astype(np.float64))
    frequency = np.where(pair < first_pairs, 0.0, power).astype(np.float32)
    return np.concatenate([frequency, frequency]).reshape(1, head_dim)


def kernel(
    nb,
    patch_ref,
    refresh_ref,
    tlen_ref,
    mod_ref,
    freq_ref,
    qg_ref,
    kg_ref,
    x_hbm,
    w_hbm,
    wo_hbm,
    tk_hbm,
    tv_hbm,
    sk_hbm,
    sv_hbm,
    cr_hbm,
    out_hbm,
    w,
    xf,
    xo,
    cr,
    xm,
    stb,
    fresh,
    rowb,
    kvb,
    textb,
    acc,
    mst,
    lst,
    osend,
    att,
    wown,
    woth,
    outv,
    lsem,
    img_s,
    img_r,
    sib_s,
    sib_r,
    st_s,
    st_r,
    txt_s,
    txt_r,
    ty_s,
    ty_r,
    y_s,
    y_r,
    f_s,
    f_r,
    a_s,
    a_r,
    w_s,
    w_r,
):
    b = lax.axis_index("batch")
    me = lax.axis_index("seq")
    h = lax.axis_index("head")
    k = me % 2
    xl = (me // 2) % 2
    y = me // 4
    mine = me % 4
    half = xo.shape[2]
    width = 2 * half
    cr_rows = xo.shape[1] // NC
    t_rows = xo.shape[1] // NT
    tile = 4 * t_rows
    hd = 128
    tw = TRI * hd
    ns = 2 * nb
    wrows = woth.shape[0] // ns
    trow = tk_hbm.shape[1]
    cexp = (hd ** -0.5) * math.log2(math.e)

    def member(rel):
        return ((xl + rel // 2) % 2) * 2 + (k + rel % 2) % 2

    def row_peer(rel, other=0):
        return {"seq": y * 4 + member(rel), "head": (h + other) % 2}

    def y_of(d):
        return (y + d) % 4

    def y_peer(d):
        return {"seq": y_of(d) * 4 + mine}

    def remote(src, dst, ss, rs, dev):
        return pltpu.make_async_remote_copy(src, dst, ss, rs, device_id=dev, device_id_type=MESH)

    def rows_of(c):
        return pl.ds(pl.multiple_of(c * cr_rows, cr_rows), cr_rows)

    def tri_cols(kk):
        return pl.ds(pl.multiple_of(kk * tw, 128), tw)

    own_off = pl.multiple_of(h * half, 128)
    part_off = pl.multiple_of((1 - h) * half, 128)

    local = [
        pltpu.make_async_copy(x_hbm.at[xl], xf.at[h, mine], lsem.at[0]),
        pltpu.make_async_copy(sk_hbm.at[xl, :, tri_cols(k)], stb.at[mine, :, 0:tw], lsem.at[1]),
        pltpu.make_async_copy(
            sv_hbm.at[xl, :, tri_cols(k)], stb.at[mine, :, tw : 2 * tw], lsem.at[2]
        ),
        pltpu.make_async_copy(
            tk_hbm.at[xl, :, tri_cols(k)], textb.at[y, mine, :, 0:tw], lsem.at[3]
        ),
        pltpu.make_async_copy(
            tv_hbm.at[xl, :, tri_cols(k)], textb.at[y, mine, :, tw : 2 * tw], lsem.at[4]
        ),
    ]
    for kind in range(3):
        local.append(
            pltpu.make_async_copy(
                w_hbm.at[kind, :, tri_cols(k)], w.at[:, kind * tw : (kind + 1) * tw], lsem.at[5 + kind]
            )
        )
    late = [
        pltpu.make_async_copy(wo_hbm.at[:, pl.ds(own_off, half)], wown, lsem.at[8]),
        pltpu.make_async_copy(cr_hbm, cr, lsem.at[9]),
        pltpu.make_async_copy(x_hbm, xo, lsem.at[10]),
    ]
    for c_ in local:
        c_.start()

    peers = [y_peer(d) for d in (2, 1, 3)]
    peers += [row_peer(r, 1) for r in range(4)]
    zpeers = []
    for db in range(nb):
        for dk in range(2):
            if db == 0 and dk == 0:
                continue
            dev = {"batch": (b + db) % nb, "seq": me + dk * (1 - 2 * k)}
            zpeers.append((db, dk, dev))
            if db != 0:
                peers.append(dev)
    peers += [row_peer(r) for r in (1, 2, 3)]
    bar = pltpu.get_barrier_semaphore()
    for p_ in peers:
        pl.semaphore_signal(bar, inc=1, device_id=p_, device_id_type=MESH)
    pl.semaphore_wait(bar, len(peers))

    def txt(rel, part):
        m = member(rel)
        return remote(
            (tk_hbm if part == 0 else tv_hbm).at[m // 2, :, tri_cols(m % 2)],
            textb.at[y, mine, :, part * tw : (part + 1) * tw],
            txt_s.at[rel],
            txt_r.at[rel],
            row_peer(rel),
        )

    def txt_arrival(rel):
        landed = textb.at[y, member(rel)]
        return remote(landed, landed, txt_s.at[rel], txt_r.at[rel], row_peer(rel))

    def img_peer(kind):
        return row_peer((1, 0, 2, 2)[kind], (0, 1, 0, 1)[kind])

    def img(c, kind):
        p = xl if kind < 2 else 1 - xl
        return remote(
            x_hbm.at[p, rows_of(c)],
            xf.at[h, mine, rows_of(c)],
            img_s.at[kind],
            img_r.at[c, kind],
            img_peer(kind),
        )

    def img_landed(c, kind):
        m = member((1, 0, 2, 2)[kind])
        return xf.at[(h + (0, 1, 0, 1)[kind]) % 2, m, rows_of(c)]

    def img_arrival(c, kind):
        d = img_landed(c, kind)
        return remote(d, d, img_s.at[kind], img_r.at[c, kind], img_peer(kind))

    def pass_on(c, kind):
        d = img_landed(c, kind)
        return remote(d, d, sib_s.at[kind - 1], sib_r.at[c, kind - 1], row_peer(1))

    def pass_arrival(c, kind):
        m = member((1, 1, 3, 3)[kind])
        d = xf.at[(h + (0, 1, 0, 1)[kind]) % 2, m, rows_of(c)]
        return remote(d, d, sib_s.at[kind - 1], sib_r.at[c, kind - 1], row_peer(1))

    def stale(c, rel, part):
        m = member(rel)
        return remote(
            (sk_hbm if part == 0 else sv_hbm).at[m // 2, rows_of(c), tri_cols(m % 2)],
            stb.at[mine, rows_of(c), part * tw : (part + 1) * tw],
            st_s.at[rel],
            st_r.at[c, rel],
            row_peer(rel),
        )

    def stale_arrival(c, rel):
        d = stb.at[member(rel), rows_of(c)]
        return remote(d, d, st_s.at[rel], st_r.at[c, rel], row_peer(rel))

    def send_image(c):
        for kind in (1, 2, 3, 0):
            img(c, kind).start()

    def send_stale(c):
        for rel in (2, 3, 1):
            for part in range(2):
                stale(c, rel, part).start()

    for rel in (2, 3, 1):
        for part in range(2):
            txt(rel, part).start()

    def send_chunk(c, carry):
        send_image(c)
        send_stale(c)
        return carry

    lax.fori_loop(0, NC, send_chunk, 0)

    def w_slot(db, dk):
        return ((b + nb - db) % nb) * 2 + (k + dk) % 2

    def w_rows(s):
        return pl.ds(pl.multiple_of(s * wrows, wrows), wrows)

    my_rows = w_rows(b * 2 + k)

    def w_pass(i):
        return remote(
            woth.at[my_rows], woth.at[my_rows], w_s.at[1 + i], w_r.at[1 + i], zpeers[i][2]
        )

    w_first = remote(
        wo_hbm.at[my_rows, pl.ds(part_off, half)],
        woth.at[my_rows],
        w_s.at[0],
        w_r.at[0],
        row_peer(2, 1),
    )
    w_first.start()
    for c_ in late:
        c_.start()

    def ty(d):
        return remote(textb.at[y], textb.at[y], ty_s.at[d - 1], ty_r.at[d - 1], y_peer(d))

    def ty_arrival(d):
        landed = textb.at[y_of(4 - d)]
        return remote(landed, landed, ty_s.at[d - 1], ty_r.at[d - 1], y_peer(4 - d))

    for c_ in local:
        c_.wait()
    for rel in (1, 2, 3):
        txt_arrival(rel).wait_recv()
    for d in (1, 3, 2):
        ty(d).start()

    def pair_of(part):
        return pl.ds(2 * ((xl + part) % 2), 2)

    def y_send(c, part, way):
        return remote(
            rowb.at[pair_of(part), rows_of(c), tw : 3 * tw],
            kvb.at[y, pair_of(part), rows_of(c)],
            y_s.at[part, way],
            y_r.at[c, part, way],
            y_peer(1 if way == 0 else 3),
        )

    def y_arrival(c, part, way):
        d = 3 if way == 0 else 1
        landed = kvb.at[y_of(d), pair_of(part), rows_of(c)]
        return remote(landed, landed, y_s.at[part, way], y_r.at[c, part, way], y_peer(d))

    def fwd(c, part):
        held = kvb.at[y_of(3 if part == 0 else 1), pair_of(part), rows_of(c)]
        return remote(
            held, held, f_s.at[part], f_r.at[c, part], y_peer(1 if part == 0 else 3)
        )

    def fwd_arrival(c, part):
        landed = kvb.at[y_of(2), pair_of(part), rows_of(c)]
        return remote(
            landed, landed, f_s.at[part], f_r.at[c, part], y_peer(3 if part == 0 else 1)
        )

    def nt(q, kv):
        return lax.dot_general(q, kv, (((1,), (1,)), ((), ())), preferred_element_type=F32)

    def lanes_of(s):
        return [s[:, i : i + hd] for i in range(0, s.shape[1], hd)]

    def fold(parts, op):
        while len(parts) > 1:
            parts = [
                op(parts[i], parts[i + 1]) if i + 1 < len(parts) else parts[i]
                for i in range(0, len(parts), 2)
            ]
        return parts[0]

    def tile_rows(c):
        return pl.ds(pl.multiple_of(c * t_rows, t_rows), t_rows)

    def query(cq, j):
        return rowb[:, tile_rows(cq), j * hd : (j + 1) * hd].reshape(tile, hd)

    def text_piece(t):
        def piece(q, j):
            span = slice(2 * t, 2 * t + 2)
            nkey = 8 * trow
            kt = textb[span, :, :, j * hd : (j + 1) * hd].reshape(nkey, hd)
            sc = nt(q, kt)
            sc = jnp.where(
                lax.broadcasted_iota(jnp.int32, sc.shape, 1) + t * nkey < tlen_ref[xl], sc, NEG
            )

            def weigh(e):
                vt = textb[span, :, :, tw + j * hd : tw + (j + 1) * hd].reshape(nkey, hd)
                return jnp.dot(e.astype(BF), vt, preferred_element_type=F32)

            return sc, weigh

        return piece

    def own_piece(ck):
        def piece(q, j):
            same = (
                lax.broadcasted_iota(jnp.int32, (tile, tile), 0) // t_rows
                == lax.broadcasted_iota(jnp.int32, (tile, tile), 1) // t_rows
            )
            kc = rowb[:, tile_rows(ck), tw + j * hd : tw + (j + 1) * hd].reshape(tile, hd)
            kf = fresh[:, tile_rows(ck), j * hd : (j + 1) * hd].reshape(tile, hd)
            sc = jnp.where(same, nt(q, kf), nt(q, kc))

            def weigh(e):
                vc = rowb[:, tile_rows(ck), 2 * tw + j * hd : 2 * tw + (j + 1) * hd].reshape(tile, hd)
                vf = fresh[:, tile_rows(ck), tw + j * hd : tw + (j + 1) * hd].reshape(tile, hd)
                return jnp.dot(
                    jnp.where(same, 0.0, e).astype(BF), vc, preferred_element_type=F32
                ) + jnp.dot(jnp.where(same, e, 0.0).astype(BF), vf, preferred_element_type=F32)

            return sc, weigh

        return piece

    def far_piece(ck, d):
        yy = y_of(d)

        def piece(q, j):
            kc = kvb[yy, :, tile_rows(ck), j * hd : (j + 1) * hd].reshape(tile, hd)

            def weigh(e):
                vc = kvb[yy, :, tile_rows(ck), tw + j * hd : tw + (j + 1) * hd].reshape(tile, hd)
                return jnp.dot(e.astype(BF), vc, preferred_element_type=F32)

            return nt(q, kc), weigh

        return piece

    def unit(lo, hi, pieces, first=False, then=None, mid=None):
        def step(cq, carry):
            for j in range(TRI):
                q = query(cq, j)
                got = [p(q, j) for p in pieces]
                top = fold([t for sc, _ in got for t in lanes_of(sc)], jnp.maximum)
                top = jnp.broadcast_to(jnp.max(top, axis=-1, keepdims=True), (tile, hd))
                if not first:
                    old = mst[cq, j]
                    top = jnp.maximum(top, old)
                ref = top * cexp
                sums, av = [], None
                for sc, weigh in got:
                    e = [jnp.exp2(t * cexp - ref) for t in lanes_of(sc)]
                    sums += e
                    add = weigh(jnp.concatenate(e, axis=1))
                    av = add if av is None else av + add
                tot = fold(sums, jnp.add)
                if not first:
                    shrink = jnp.exp2(old * cexp - ref)
                    tot = tot + lst[cq, j] * shrink
                    av = av + acc[cq, j] * shrink
                if then is None:
                    mst[cq, j] = top
                    lst[cq, j] = tot
                    acc[cq, j] = av
                else:
                    then(cq, j, tot, av)
            if then is not None:
                then(cq, None, None, None)
            if mid is not None:
                pl.when(cq == lo)(lambda: relay(mid))
            return carry

        lax.fori_loop(lo, hi, step, 0)

    text = [text_piece(0), text_piece(1)]

    def near(*cks):
        return [far_piece(ck, d) for ck in cks for d in (3, 1)]

    def opp(*cks):
        return [far_piece(ck, 2) for ck in cks]

    def own(*cks):
        return [own_piece(ck) for ck in cks]

    def opp_wait(c):
        fwd_arrival(c, 0).wait_recv()
        fwd_arrival(c, 1).wait_recv()

    lane = lax.broadcasted_iota(jnp.int32, (cr_rows, hd), 1) % (hd // 2)
    col = lax.broadcasted_iota(jnp.int32, (cr_rows, hd), 0).astype(F32)
    freq = freq_ref[...]
    first_pairs = hd // 16
    axis_pairs = (hd // 2 - first_pairs) // 2
    is_row = lane < first_pairs + axis_pairs
    low = lax.broadcasted_iota(jnp.int32, (cr_rows, hd), 1) < hd // 2

    def relay(c):
        for kind in (1, 2, 3):
            img_arrival(c, kind).wait_recv()
            pass_on(c, kind).start()

    def qkv_step(c, carry):
        @pl.when(c < 4)
        def _():
            relay(c)

        img_arrival(c, 0).wait_recv()
        for kind in (1, 2, 3):
            pass_arrival(c, kind).wait_recv()
        rows = rows_of(c)
        for m in range(4):
            a = xf[0, m, rows, :].astype(F32)
            d = xf[1, m, rows, :].astype(F32)
            total = jnp.sum(a, axis=-1, keepdims=True) + jnp.sum(d, axis=-1, keepdims=True)
            mean = total / width
            a = a - mean
            d = d - mean
            var = (
                jnp.sum(a * a, axis=-1, keepdims=True) + jnp.sum(d * d, axis=-1, keepdims=True)
            ) / width
            inv = lax.rsqrt(var + EPS)
            for i, v in enumerate((a, d)):
                scale = 1.0 + mod_ref[1, pl.ds(xl, 1), i * half : (i + 1) * half]
                shift = mod_ref[0, pl.ds(xl, 1), i * half : (i + 1) * half]
                xm[m * cr_rows : (m + 1) * cr_rows, i * half : (i + 1) * half] = (
                    v * inv * scale + shift
                ).astype(BF)
        cosv, sinv = [], []
        for m in range(4):
            raster = patch_ref[y * 4 + m] * (NC * cr_rows) + c * cr_rows
            row_pos = (raster // GRID_W).astype(F32)
            col_pos = (raster % GRID_W).astype(F32) + col
            angle = jnp.where(is_row, row_pos, col_pos) * freq
            cosv.append(jnp.cos(angle))
            sine = jnp.sin(angle)
            sinv.append(jnp.where(low, -sine, sine))
        cosv = jnp.concatenate(cosv, axis=0)
        sinv = jnp.concatenate(sinv, axis=0)
        for kind in range(3):
            proj = jnp.dot(
                xm[...], w[:, kind * tw : (kind + 1) * tw], preferred_element_type=F32
            )
            for j in range(TRI):
                t = proj[:, j * hd : (j + 1) * hd]
                if kind < 2:
                    gain = (qg_ref if kind == 0 else kg_ref)[...]
                    ms = jnp.mean(t * t, axis=-1, keepdims=True)
                    t = t * lax.rsqrt(ms + EPS) * gain
                    t = t * cosv + pltpu.roll(t, hd // 2, 1) * sinv
                t = t.astype(BF)
                at = kind * tw + j * hd
                for m in range(4):
                    piece = t[m * cr_rows : (m + 1) * cr_rows]
                    if kind == 0:
                        rowb[m, rows, at : at + hd] = piece
                    else:
                        fresh[m, rows, at - tw : at - tw + hd] = piece
        for rel in (1, 2, 3):
            stale_arrival(c, rel).wait_recv()
        for m in range(4):
            rowb[m, rows, tw : 3 * tw] = jnp.where(
                refresh_ref[y * 4 + m] == 1, fresh[m, rows, :], stb[m, rows, :]
            )
        for part, way in ((0, 0), (1, 1), (1, 0), (0, 1)):
            y_send(c, part, way).start()

        @pl.when(c == 1)
        def _():
            for d in (1, 2, 3):
                ty_arrival(d).wait_recv()
            unit(0, 1, text + own(0), first=True)

        @pl.when(c >= 1)
        def _():
            y_arrival(c - 1, 0, 0).wait_recv()
            fwd(c - 1, 0).start()
            y_arrival(c - 1, 1, 1).wait_recv()
            fwd(c - 1, 1).start()
            y_arrival(c - 1, 1, 0).wait_recv()
            y_arrival(c - 1, 0, 1).wait_recv()

        @pl.when(c == 3)
        def _():
            unit(1, 2, text + own(0, 1), first=True)
            relay(4)
            unit(0, 1, own(1))

        @pl.when(c == 4)
        def _():
            unit(0, 2, near(0, 1), mid=5)

        @pl.when(c == 5)
        def _():
            unit(2, 3, text + own(0, 1, 2), first=True)
            relay(6)

        @pl.when(c == 6)
        def _():
            w_first.wait_recv()
            for i in range(len(zpeers)):
                w_pass(i).start()
            for e in range(4):
                opp_wait(e)
            unit(0, 2, opp(0, 1), mid=7)

        return carry

    lax.fori_loop(0, NC, qkv_step, 0)

    unit(2, 3, own(3) + near(0, 1) + opp(0, 1))
    unit(0, 2, own(2, 3) + near(2))
    y_arrival(NC - 1, 0, 0).wait_recv()
    fwd(NC - 1, 0).start()
    y_arrival(NC - 1, 1, 1).wait_recv()
    fwd(NC - 1, 1).start()
    y_arrival(NC - 1, 1, 0).wait_recv()
    y_arrival(NC - 1, 0, 1).wait_recv()
    unit(0, 2, near(3))
    unit(3, 4, text + own(0), first=True)
    for e in range(4, NC):
        opp_wait(e)

    def att_slot(hh, m, c):
        at = pl.multiple_of((c % 2) * t_rows, t_rows)
        return att.at[hh, m % 2, c // 2, m // 2, pl.ds(at, t_rows)]

    def a_send(c, rel, other):
        i = rel * 2 + other
        return remote(
            osend.at[member(rel), c],
            att_slot(h, mine, c),
            a_s.at[i],
            a_r.at[c, i],
            row_peer(rel, other),
        )

    def a_arrival(c, rel, other):
        i = rel * 2 + other
        d = att_slot((h + other) % 2, member(rel), c)
        return remote(d, d, a_s.at[i], a_r.at[c, i], row_peer(rel, other))

    far_order = ((2, 1), (0, 1), (3, 1), (1, 1), (2, 0), (3, 0), (1, 0))

    def deliver(cq, j, tot, av):
        if j is not None:
            o = (av / jnp.sum(tot, axis=-1, keepdims=True)).astype(BF)
            for m in range(4):
                osend[m, cq, :, j * hd : (j + 1) * hd] = o[m * t_rows : (m + 1) * t_rows]
            return
        for rel, other in far_order:
            a_send(cq, rel, other).start()
        at = pl.multiple_of((cq % 2) * t_rows, t_rows)
        att[h, k, cq // 2, xl, pl.ds(at, t_rows)] = osend[mine, cq]

    unit(0, 2, opp(2, 3), then=deliver)
    unit(2, 3, near(2, 3) + opp(2, 3), then=deliver)
    unit(3, 4, own(1, 2, 3) + near(0, 1))
    unit(3, 4, near(2, 3) + opp(0, 1, 2, 3), then=deliver)

    for c_ in late:
        c_.wait()
    for i, (db, dk, dev) in enumerate(zpeers):
        rows = w_rows(w_slot(db, dk))
        remote(woth.at[rows], woth.at[rows], w_s.at[1 + i], w_r.at[1 + i], dev).wait_recv()

    def out_copy(s, p):
        rows = pl.ds(pl.multiple_of(s * 2 * t_rows, t_rows), 2 * t_rows)
        return pltpu.make_async_copy(outv.at[p, rows], out_hbm.at[p, rows], lsem.at[11 + 2 * s + p])

    def finish(s, carry):
        for rel, other in far_order[::-1]:
            for e in range(2):
                a_arrival(2 * s + e, rel, other).wait_recv()
        proj = None
        for i, wref in enumerate((wown, woth)):
            hh = (h + i) % 2
            for kk in range(2):
                lhs = att[hh, kk, s].reshape(tile, tw)
                part = jnp.dot(
                    lhs, wref[kk * tw : (kk + 1) * tw, :], preferred_element_type=F32
                )
                proj = part if proj is None else proj + part
        rows = pl.ds(pl.multiple_of(s * 2 * t_rows, t_rows), 2 * t_rows)
        for p in range(2):
            gate = mod_ref[2, pl.ds(p, 1), pl.ds(own_off, half)]
            outv[p, rows, :] = (
                xo[p, rows, :].astype(F32)
                + gate * proj[p * 2 * t_rows : (p + 1) * 2 * t_rows]
                + cr[p, rows, :].astype(F32)
            ).astype(BF)
            out_copy(s, p).start()
        return carry

    lax.fori_loop(0, 2, finish, 0)

    for s in range(2):
        for p in range(2):
            out_copy(s, p).wait()

    def sent(buf, sem):
        remote(buf, buf, sem, sem, row_peer(1)).wait_send()

    for kind in range(4):
        sent(xf.at[0, 0], img_s.at[kind])
    for kind in range(3):
        sent(xf.at[0, 0], sib_s.at[kind])
    for rel in (1, 2, 3):
        sent(stb.at[0], st_s.at[rel])
        sent(textb.at[0, 0], txt_s.at[rel])
    for part in range(2):
        for way in range(2):
            sent(kvb.at[0, 0:2], y_s.at[part, way])
        sent(kvb.at[0, 0:2], f_s.at[part])
    for rel, other in far_order:
        sent(osend.at[0], a_s.at[rel * 2 + other])
    for d in (1, 2, 3):
        ty(d).wait_send()
    w_first.wait_send()
    for i in range(len(zpeers)):
        w_pass(i).wait_send()


def per_device(
    nb,
    image_hidden,
    modulation,
    qkv_weight,
    out_weight,
    q_gain,
    k_gain,
    text_keys,
    text_values,
    stale_keys,
    stale_values,
    cached_residual,
    patch_of,
    refresh,
    text_len,
):
    prompts, rows, half = image_hidden.shape
    hd = q_gain.shape[0]
    channels = out_weight.shape[0]
    tw = TRI * hd
    cr_rows = rows // NC
    t_rows = rows // NT
    trow = text_keys.shape[1]
    smem = pl.BlockSpec(memory_space=pltpu.SMEM)
    vmem = pl.BlockSpec(memory_space=pltpu.VMEM)
    hbm = pl.BlockSpec(memory_space=pl.ANY)
    dma = pltpu.SemaphoreType.DMA
    ns = 2 * nb
    return pl.pallas_call(
        functools.partial(kernel, nb),
        name="joint",
        out_shape=jax.ShapeDtypeStruct(image_hidden.shape, BF),
        in_specs=[smem] * 3 + [vmem] * 4 + [hbm] * 8,
        out_specs=hbm,
        scratch_shapes=[
            pltpu.VMEM((2 * half, 3 * tw), BF),
            pltpu.VMEM((2, 4, rows, half), BF),
            pltpu.VMEM((prompts, rows, half), BF),
            pltpu.VMEM((prompts, rows, half), BF),
            pltpu.VMEM((4 * cr_rows, 2 * half), BF),
            pltpu.VMEM((4, rows, 2 * tw), BF),
            pltpu.VMEM((4, rows, 2 * tw), BF),
            pltpu.VMEM((4, rows, 3 * tw), BF),
            pltpu.VMEM((4, 4, rows, 2 * tw), BF),
            pltpu.VMEM((4, 4, trow, 2 * tw), BF),
            pltpu.VMEM((NT, TRI, 4 * t_rows, hd), F32),
            pltpu.VMEM((NT, TRI, 4 * t_rows, hd), F32),
            pltpu.VMEM((NT, TRI, 4 * t_rows, hd), F32),
            pltpu.VMEM((4, NT, t_rows, tw), BF),
            pltpu.VMEM((2, 2, 2, 2, 2 * t_rows, tw), BF),
            pltpu.VMEM((channels, half), BF),
            pltpu.VMEM((channels, half), BF),
            pltpu.VMEM((prompts, rows, half), BF),
            dma((15,)),
            dma((4,)),
            dma((NC, 4)),
            dma((3,)),
            dma((NC, 3)),
            dma((4,)),
            dma((NC, 4)),
            dma((4,)),
            dma((4,)),
            dma((3,)),
            dma((3,)),
            dma((2, 2)),
            dma((NC, 2, 2)),
            dma((2,)),
            dma((NC, 2)),
            dma((8,)),
            dma((NT, 8)),
            dma((ns,)),
            dma((ns,)),
        ],
        compiler_params=pltpu.CompilerParams(
            collective_id=0, has_side_effects=True, vmem_limit_bytes=66 * 1024 * 1024 - 2097152
        ),
    )(
        patch_of,
        refresh,
        text_len,
        jnp.transpose(modulation, (1, 0, 2)),
        jnp.asarray(pair_frequency(hd)),
        q_gain.reshape(1, hd),
        k_gain.reshape(1, hd),
        image_hidden,
        jnp.transpose(qkv_weight, (1, 0, 2)),
        out_weight,
        text_keys,
        text_values,
        stale_keys,
        stale_values,
        cached_residual,
    )


def solution(mesh):
    in_specs = (
        P("batch", "seq", "head"),
        P("batch", None, None),
        P(None, None, "head"),
        P("head", None),
        P(),
        P(),
        P("batch", "seq", "head"),
        P("batch", "seq", "head"),
        P("batch", "seq", "head"),
        P("batch", "seq", "head"),
        P("batch", "seq", "head"),
        P("batch"),
        P("batch"),
        P("batch"),
    )
    out_specs = P("batch", "seq", "head")
    return jax.shard_map(
        functools.partial(per_device, mesh.shape["batch"]),
        mesh=mesh,
        in_specs=in_specs,
        out_specs=out_specs,
        check_vma=False,
    )
```

```python
import functools
import math

import jax
import jax.numpy as jnp
import numpy as np
from jax import lax
from jax.experimental import pallas as pl
from jax.experimental.pallas import tpu as pltpu
from jax.sharding import PartitionSpec as P

GRID_W = 64
EPS = 1e-06
NEG = -1e30
MESH = pl.DeviceIdType.MESH
BF = jnp.bfloat16
F32 = jnp.float32

NC = 8
NT = 4
TRI = 3


def pair_frequency(head_dim):
    half_dim = head_dim // 2
    first_pairs = head_dim // 16
    axis_pairs = (half_dim - first_pairs) // 2
    pair = np.arange(half_dim)
    local = np.where(pair < first_pairs + axis_pairs, pair - first_pairs, pair - first_pairs - axis_pairs)
    exponent = -local.astype(np.float32) / np.float32(axis_pairs)
    power = np.power(10000.0, exponent.astype(np.float64))
    frequency = np.where(pair < first_pairs, 0.0, power).astype(np.float32)
    return np.concatenate([frequency, frequency]).reshape(1, head_dim)


def kernel(
    nb,
    patch_ref,
    refresh_ref,
    tlen_ref,
    mod_ref,
    freq_ref,
    qg_ref,
    kg_ref,
    x_hbm,
    w_hbm,
    wo_hbm,
    tk_hbm,
    tv_hbm,
    sk_hbm,
    sv_hbm,
    cr_hbm,
    out_hbm,
    w,
    xf,
    xo,
    cr,
    xm,
    stb,
    fresh,
    rowb,
    kvb,
    textb,
    acc,
    mst,
    lst,
    osend,
    att,
    wown,
    woth,
    outv,
    lsem,
    img_s,
    img_r,
    sib_s,
    sib_r,
    st_s,
    st_r,
    txt_s,
    txt_r,
    ty_s,
    ty_r,
    y_s,
    y_r,
    f_s,
    f_r,
    a_s,
    a_r,
    w_s,
    w_r,
):
    b = lax.axis_index("batch")
    me = lax.axis_index("seq")
    h = lax.axis_index("head")
    k = me % 2
    xl = (me // 2) % 2
    y = me // 4
    mine = me % 4
    half = xo.shape[2]
    width = 2 * half
    cr_rows = xo.shape[1] // NC
    t_rows = xo.shape[1] // NT
    tile = 4 * t_rows
    hd = 128
    tw = TRI * hd
    ns = 2 * nb
    wrows = woth.shape[0] // ns
    trow = tk_hbm.shape[1]
    cexp = (hd ** -0.5) * math.log2(math.e)

    def member(rel):
        return ((xl + rel // 2) % 2) * 2 + (k + rel % 2) % 2

    def row_peer(rel, other=0):
        return {"seq": y * 4 + member(rel), "head": (h + other) % 2}

    def y_of(d):
        return (y + d) % 4

    def y_peer(d):
        return {"seq": y_of(d) * 4 + mine}

    def remote(src, dst, ss, rs, dev):
        return pltpu.make_async_remote_copy(src, dst, ss, rs, device_id=dev, device_id_type=MESH)

    def rows_of(c):
        return pl.ds(pl.multiple_of(c * cr_rows, cr_rows), cr_rows)

    def tri_cols(kk):
        return pl.ds(pl.multiple_of(kk * tw, 128), tw)

    own_off = pl.multiple_of(h * half, 128)
    part_off = pl.multiple_of((1 - h) * half, 128)

    local = [
        pltpu.make_async_copy(x_hbm.at[xl], xf.at[h, mine], lsem.at[0]),
        pltpu.make_async_copy(sk_hbm.at[xl, :, tri_cols(k)], stb.at[mine, :, 0:tw], lsem.at[1]),
        pltpu.make_async_copy(
            sv_hbm.at[xl, :, tri_cols(k)], stb.at[mine, :, tw : 2 * tw], lsem.at[2]
        ),
        pltpu.make_async_copy(
            tk_hbm.at[xl, :, tri_cols(k)], textb.at[y, mine, :, 0:tw], lsem.at[3]
        ),
        pltpu.make_async_copy(
            tv_hbm.at[xl, :, tri_cols(k)], textb.at[y, mine, :, tw : 2 * tw], lsem.at[4]
        ),
    ]
    for kind in range(3):
        local.append(
            pltpu.make_async_copy(
                w_hbm.at[kind, :, tri_cols(k)], w.at[:, kind * tw : (kind + 1) * tw], lsem.at[5 + kind]
            )
        )
    late = [
        pltpu.make_async_copy(wo_hbm.at[:, pl.ds(own_off, half)], wown, lsem.at[8]),
        pltpu.make_async_copy(cr_hbm, cr, lsem.at[9]),
        pltpu.make_async_copy(x_hbm, xo, lsem.at[10]),
    ]
    for c_ in local:
        c_.start()

    peers = [y_peer(d) for d in (2, 1, 3)]
    peers += [row_peer(r, 1) for r in range(4)]
    zpeers = []
    for db in range(nb):
        for dk in range(2):
            if db == 0 and dk == 0:
                continue
            dev = {"batch": (b + db) % nb, "seq": me + dk * (1 - 2 * k)}
            zpeers.append((db, dk, dev))
            if db != 0:
                peers.append(dev)
    peers += [row_peer(r) for r in (1, 2, 3)]
    bar = pltpu.get_barrier_semaphore()
    for p_ in peers:
        pl.semaphore_signal(bar, inc=1, device_id=p_, device_id_type=MESH)
    pl.semaphore_wait(bar, len(peers))

    def txt(rel, part):
        m = member(rel)
        return remote(
            (tk_hbm if part == 0 else tv_hbm).at[m // 2, :, tri_cols(m % 2)],
            textb.at[y, mine, :, part * tw : (part + 1) * tw],
            txt_s.at[rel],
            txt_r.at[rel],
            row_peer(rel),
        )

    def txt_arrival(rel):
        landed = textb.at[y, member(rel)]
        return remote(landed, landed, txt_s.at[rel], txt_r.at[rel], row_peer(rel))

    def img_peer(kind):
        return row_peer((1, 0, 2, 2)[kind], (0, 1, 0, 1)[kind])

    def img(c, kind):
        p = xl if kind < 2 else 1 - xl
        return remote(
            x_hbm.at[p, rows_of(c)],
            xf.at[h, mine, rows_of(c)],
            img_s.at[kind],
            img_r.at[c, kind],
            img_peer(kind),
        )

    def img_landed(c, kind):
        m = member((1, 0, 2, 2)[kind])
        return xf.at[(h + (0, 1, 0, 1)[kind]) % 2, m, rows_of(c)]

    def img_arrival(c, kind):
        d = img_landed(c, kind)
        return remote(d, d, img_s.at[kind], img_r.at[c, kind], img_peer(kind))

    def pass_on(c, kind):
        d = img_landed(c, kind)
        return remote(d, d, sib_s.at[kind - 1], sib_r.at[c, kind - 1], row_peer(1))

    def pass_arrival(c, kind):
        m = member((1, 1, 3, 3)[kind])
        d = xf.at[(h + (0, 1, 0, 1)[kind]) % 2, m, rows_of(c)]
        return remote(d, d, sib_s.at[kind - 1], sib_r.at[c, kind - 1], row_peer(1))

    def stale(c, rel, part):
        m = member(rel)
        return remote(
            (sk_hbm if part == 0 else sv_hbm).at[m // 2, rows_of(c), tri_cols(m % 2)],
            stb.at[mine, rows_of(c), part * tw : (part + 1) * tw],
            st_s.at[rel],
            st_r.at[c, rel],
            row_peer(rel),
        )

    def stale_arrival(c, rel):
        d = stb.at[member(rel), rows_of(c)]
        return remote(d, d, st_s.at[rel], st_r.at[c, rel], row_peer(rel))

    def send_image(c):
        for kind in (1, 2, 3, 0):
            img(c, kind).start()

    def send_stale(c):
        for rel in (2, 3, 1):
            for part in range(2):
                stale(c, rel, part).start()

    for rel in (2, 3, 1):
        for part in range(2):
            txt(rel, part).start()

    def send_chunk(c, carry):
        send_image(c)
        send_stale(c)
        return carry

    lax.fori_loop(0, NC, send_chunk, 0)

    def w_slot(db, dk):
        return ((b + nb - db) % nb) * 2 + (k + dk) % 2

    def w_rows(s):
        return pl.ds(pl.multiple_of(s * wrows, wrows), wrows)

    my_rows = w_rows(b * 2 + k)

    def w_pass(i):
        return remote(
            woth.at[my_rows], woth.at[my_rows], w_s.at[1 + i], w_r.at[1 + i], zpeers[i][2]
        )

    w_first = remote(
        wo_hbm.at[my_rows, pl.ds(part_off, half)],
        woth.at[my_rows],
        w_s.at[0],
        w_r.at[0],
        row_peer(2, 1),
    )
    w_first.start()
    for c_ in late:
        c_.start()

    def ty(d):
        return remote(textb.at[y], textb.at[y], ty_s.at[d - 1], ty_r.at[d - 1], y_peer(d))

    def ty_arrival(d):
        landed = textb.at[y_of(4 - d)]
        return remote(landed, landed, ty_s.at[d - 1], ty_r.at[d - 1], y_peer(4 - d))

    for c_ in local:
        c_.wait()
    for rel in (1, 2, 3):
        txt_arrival(rel).wait_recv()
    for d in (1, 3, 2):
        ty(d).start()

    def pair_of(part):
        return pl.ds(2 * ((xl + part) % 2), 2)

    def y_send(c, part, way):
        return remote(
            rowb.at[pair_of(part), rows_of(c), tw : 3 * tw],
            kvb.at[y, pair_of(part), rows_of(c)],
            y_s.at[part, way],
            y_r.at[c, part, way],
            y_peer(1 if way == 0 else 3),
        )

    def y_arrival(c, part, way):
        d = 3 if way == 0 else 1
        landed = kvb.at[y_of(d), pair_of(part), rows_of(c)]
        return remote(landed, landed, y_s.at[part, way], y_r.at[c, part, way], y_peer(d))

    def fwd(c, part):
        held = kvb.at[y_of(3 if part == 0 else 1), pair_of(part), rows_of(c)]
        return remote(
            held, held, f_s.at[part], f_r.at[c], y_peer(1 if part == 0 else 3)
        )

    def fwd_arrival(c):
        landed = kvb.at[y_of(2), :, rows_of(c)]
        return remote(landed, landed, f_s.at[0], f_r.at[c], y_peer(3))

    def nt(q, kv):
        return lax.dot_general(q, kv, (((1,), (1,)), ((), ())), preferred_element_type=F32)

    def lanes_of(s):
        return [s[:, i : i + hd] for i in range(0, s.shape[1], hd)]

    def fold(parts, op):
        while len(parts) > 1:
            parts = [
                op(parts[i], parts[i + 1]) if i + 1 < len(parts) else parts[i]
                for i in range(0, len(parts), 2)
            ]
        return parts[0]

    def tile_rows(c):
        return pl.ds(pl.multiple_of(c * t_rows, t_rows), t_rows)

    def query(cq, j):
        return rowb[:, tile_rows(cq), j * hd : (j + 1) * hd].reshape(tile, hd)

    def text_piece(t):
        def piece(q, j):
            span = slice(2 * t, 2 * t + 2)
            nkey = 8 * trow
            kt = textb[span, :, :, j * hd : (j + 1) * hd].reshape(nkey, hd)
            sc = nt(q, kt)
            sc = jnp.where(
                lax.broadcasted_iota(jnp.int32, sc.shape, 1) + t * nkey < tlen_ref[xl], sc, NEG
            )

            def weigh(e):
                vt = textb[span, :, :, tw + j * hd : tw + (j + 1) * hd].reshape(nkey, hd)
                return jnp.dot(e.astype(BF), vt, preferred_element_type=F32)

            return sc, weigh

        return piece

    def own_piece(ck):
        def piece(q, j):
            same = (
                lax.broadcasted_iota(jnp.int32, (tile, tile), 0) // t_rows
                == lax.broadcasted_iota(jnp.int32, (tile, tile), 1) // t_rows
            )
            kc = rowb[:, tile_rows(ck), tw + j * hd : tw + (j + 1) * hd].reshape(tile, hd)
            kf = fresh[:, tile_rows(ck), j * hd : (j + 1) * hd].reshape(tile, hd)
            sc = jnp.where(same, nt(q, kf), nt(q, kc))

            def weigh(e):
                vc = rowb[:, tile_rows(ck), 2 * tw + j * hd : 2 * tw + (j + 1) * hd].reshape(tile, hd)
                vf = fresh[:, tile_rows(ck), tw + j * hd : tw + (j + 1) * hd].reshape(tile, hd)
                return jnp.dot(
                    jnp.where(same, 0.0, e).astype(BF), vc, preferred_element_type=F32
                ) + jnp.dot(jnp.where(same, e, 0.0).astype(BF), vf, preferred_element_type=F32)

            return sc, weigh

        return piece

    def far_piece(ck, d):
        yy = y_of(d)

        def piece(q, j):
            kc = kvb[yy, :, tile_rows(ck), j * hd : (j + 1) * hd].reshape(tile, hd)

            def weigh(e):
                vc = kvb[yy, :, tile_rows(ck), tw + j * hd : tw + (j + 1) * hd].reshape(tile, hd)
                return jnp.dot(e.astype(BF), vc, preferred_element_type=F32)

            return nt(q, kc), weigh

        return piece

    def unit(lo, hi, pieces, first=False, then=None, mid=None):
        def step(cq, carry):
            for j in range(TRI):
                q = query(cq, j)
                got = [p(q, j) for p in pieces]
                top = fold([t for sc, _ in got for t in lanes_of(sc)], jnp.maximum)
                top = jnp.broadcast_to(jnp.max(top, axis=-1, keepdims=True), (tile, hd))
                if not first:
                    old = mst[cq, j]
                    top = jnp.maximum(top, old)
                ref = top * cexp
                sums, av = [], None
                for sc, weigh in got:
                    e = [jnp.exp2(t * cexp - ref) for t in lanes_of(sc)]
                    sums += e
                    add = weigh(jnp.concatenate(e, axis=1))
                    av = add if av is None else av + add
                tot = fold(sums, jnp.add)
                if not first:
                    shrink = jnp.exp2(old * cexp - ref)
                    tot = tot + lst[cq, j] * shrink
                    av = av + acc[cq, j] * shrink
                if then is None:
                    mst[cq, j] = top
                    lst[cq, j] = tot
                    acc[cq, j] = av
                else:
                    then(cq, j, tot, av)
            if then is not None:
                then(cq, None, None, None)
            if mid is not None:
                pl.when(cq == lo)(lambda: relay(mid))
            return carry

        lax.fori_loop(lo, hi, step, 0)

    text = [text_piece(0), text_piece(1)]

    def near(*cks):
        return [far_piece(ck, d) for ck in cks for d in (3, 1)]

    def opp(*cks):
        return [far_piece(ck, 2) for ck in cks]

    def own(*cks):
        return [own_piece(ck) for ck in cks]

    def opp_wait(c):
        fwd_arrival(c).wait_recv()

    lane = lax.broadcasted_iota(jnp.int32, (cr_rows, hd), 1) % (hd // 2)
    col = lax.broadcasted_iota(jnp.int32, (cr_rows, hd), 0).astype(F32)
    freq = freq_ref[...]
    first_pairs = hd // 16
    axis_pairs = (hd // 2 - first_pairs) // 2
    is_row = lane < first_pairs + axis_pairs
    low = lax.broadcasted_iota(jnp.int32, (cr_rows, hd), 1) < hd // 2

    def relay(c):
        for kind in (1, 2, 3):
            img_arrival(c, kind).wait_recv()
            pass_on(c, kind).start()

    def qkv_step(c, carry):
        @pl.when(c < 4)
        def _():
            relay(c)

        img_arrival(c, 0).wait_recv()
        for kind in (1, 2, 3):
            pass_arrival(c, kind).wait_recv()
        rows = rows_of(c)
        for m in range(4):
            a = xf[0, m, rows, :].astype(F32)
            d = xf[1, m, rows, :].astype(F32)
            total = jnp.sum(a, axis=-1, keepdims=True) + jnp.sum(d, axis=-1, keepdims=True)
            mean = total / width
            a = a - mean
            d = d - mean
            var = (
                jnp.sum(a * a, axis=-1, keepdims=True) + jnp.sum(d * d, axis=-1, keepdims=True)
            ) / width
            inv = lax.rsqrt(var + EPS)
            for i, v in enumerate((a, d)):
                scale = 1.0 + mod_ref[1, pl.ds(xl, 1), i * half : (i + 1) * half]
                shift = mod_ref[0, pl.ds(xl, 1), i * half : (i + 1) * half]
                xm[m * cr_rows : (m + 1) * cr_rows, i * half : (i + 1) * half] = (
                    v * inv * scale + shift
                ).astype(BF)
        cosv, sinv = [], []
        for m in range(4):
            raster = patch_ref[y * 4 + m] * (NC * cr_rows) + c * cr_rows
            row_pos = (raster // GRID_W).astype(F32)
            col_pos = (raster % GRID_W).astype(F32) + col
            angle = jnp.where(is_row, row_pos, col_pos) * freq
            cosv.append(jnp.cos(angle))
            sine = jnp.sin(angle)
            sinv.append(jnp.where(low, -sine, sine))
        cosv = jnp.concatenate(cosv, axis=0)
        sinv = jnp.concatenate(sinv, axis=0)
        for kind in range(3):
            proj = jnp.dot(
                xm[...], w[:, kind * tw : (kind + 1) * tw], preferred_element_type=F32
            )
            for j in range(TRI):
                t = proj[:, j * hd : (j + 1) * hd]
                if kind < 2:
                    gain = (qg_ref if kind == 0 else kg_ref)[...]
                    ms = jnp.mean(t * t, axis=-1, keepdims=True)
                    t = t * lax.rsqrt(ms + EPS) * gain
                    t = t * cosv + pltpu.roll(t, hd // 2, 1) * sinv
                t = t.astype(BF)
                at = kind * tw + j * hd
                for m in range(4):
                    piece = t[m * cr_rows : (m + 1) * cr_rows]
                    if kind == 0:
                        rowb[m, rows, at : at + hd] = piece
                    else:
                        fresh[m, rows, at - tw : at - tw + hd] = piece
        for rel in (1, 2, 3):
            stale_arrival(c, rel).wait_recv()
        for m in range(4):
            rowb[m, rows, tw : 3 * tw] = jnp.where(
                refresh_ref[y * 4 + m] == 1, fresh[m, rows, :], stb[m, rows, :]
            )
        for part, way in ((0, 0), (1, 1), (1, 0), (0, 1)):
            y_send(c, part, way).start()

        @pl.when(c == 1)
        def _():
            for d in (1, 2, 3):
                ty_arrival(d).wait_recv()
            unit(0, 1, text + own(0), first=True)

        @pl.when(c >= 1)
        def _():
            y_arrival(c - 1, 0, 0).wait_recv()
            fwd(c - 1, 0).start()
            y_arrival(c - 1, 1, 1).wait_recv()
            fwd(c - 1, 1).start()
            y_arrival(c - 1, 1, 0).wait_recv()
            y_arrival(c - 1, 0, 1).wait_recv()

        @pl.when(c == 3)
        def _():
            unit(1, 2, text + own(0, 1), first=True)
            relay(4)
            unit(0, 1, own(1))

        @pl.when(c == 4)
        def _():
            unit(0, 2, near(0, 1), mid=5)

        @pl.when(c == 5)
        def _():
            unit(2, 3, text + own(0, 1, 2), first=True)
            relay(6)

        @pl.when(c == 6)
        def _():
            w_first.wait_recv()
            for i in range(len(zpeers)):
                w_pass(i).start()
            for e in range(4):
                opp_wait(e)
            unit(0, 2, opp(0, 1), mid=7)

        return carry

    lax.fori_loop(0, NC, qkv_step, 0)

    unit(2, 3, own(3) + near(0, 1) + opp(0, 1))
    unit(0, 2, own(2, 3) + near(2))
    y_arrival(NC - 1, 0, 0).wait_recv()
    fwd(NC - 1, 0).start()
    y_arrival(NC - 1, 1, 1).wait_recv()
    fwd(NC - 1, 1).start()
    y_arrival(NC - 1, 1, 0).wait_recv()
    y_arrival(NC - 1, 0, 1).wait_recv()
    unit(0, 2, near(3))
    unit(3, 4, text + own(0), first=True)
    for e in range(4, NC):
        opp_wait(e)

    def att_slot(hh, m, c):
        at = pl.multiple_of((c % 2) * t_rows, t_rows)
        return att.at[hh, m % 2, c // 2, m // 2, pl.ds(at, t_rows)]

    def a_send(c, rel, other):
        i = rel * 2 + other
        return remote(
            osend.at[member(rel), c],
            att_slot(h, mine, c),
            a_s.at[i],
            a_r.at[c // 2, i],
            row_peer(rel, other),
        )

    def a_arrival(s, rel, other):
        i = rel * 2 + other
        m = member(rel)
        d = att.at[(h + other) % 2, m % 2, s, m // 2]
        return remote(d, d, a_s.at[i], a_r.at[s, i], row_peer(rel, other))

    far_order = ((2, 1), (0, 1), (3, 1), (1, 1), (2, 0), (3, 0), (1, 0))

    def deliver(cq, j, tot, av):
        if j is not None:
            o = (av / jnp.sum(tot, axis=-1, keepdims=True)).astype(BF)
            for m in range(4):
                osend[m, cq, :, j * hd : (j + 1) * hd] = o[m * t_rows : (m + 1) * t_rows]
            return
        for rel, other in far_order:
            a_send(cq, rel, other).start()
        at = pl.multiple_of((cq % 2) * t_rows, t_rows)
        att[h, k, cq // 2, xl, pl.ds(at, t_rows)] = osend[mine, cq]

    unit(0, 2, opp(2, 3), then=deliver)
    unit(2, 3, near(2, 3) + opp(2, 3), then=deliver)
    unit(3, 4, own(1, 2, 3) + near(0, 1))
    unit(3, 4, near(2, 3) + opp(0, 1, 2, 3), then=deliver)

    for c_ in late:
        c_.wait()
    for i, (db, dk, dev) in enumerate(zpeers):
        rows = w_rows(w_slot(db, dk))
        remote(woth.at[rows], woth.at[rows], w_s.at[1 + i], w_r.at[1 + i], dev).wait_recv()

    def out_copy(s, p):
        rows = pl.ds(pl.multiple_of(s * 2 * t_rows, t_rows), 2 * t_rows)
        return pltpu.make_async_copy(outv.at[p, rows], out_hbm.at[p, rows], lsem.at[11 + 2 * s + p])

    def finish(s, carry):
        proj = None
        for rel, other in ((0, 1), (0, 0), (1, 1), (1, 0)):
            if (rel, other) != (0, 0):
                a_arrival(s, rel, other).wait_recv()
            a_arrival(s, rel + 2, other).wait_recv()
            kk = member(rel) % 2
            part = jnp.dot(
                att[(h + other) % 2, kk, s].reshape(tile, tw),
                (wown, woth)[other][tri_cols(kk), :],
                preferred_element_type=F32,
            )
            proj = part if proj is None else proj + part
        rows = pl.ds(pl.multiple_of(s * 2 * t_rows, t_rows), 2 * t_rows)
        for p in range(2):
            gate = mod_ref[2, pl.ds(p, 1), pl.ds(own_off, half)]
            outv[p, rows, :] = (
                xo[p, rows, :].astype(F32)
                + gate * proj[p * 2 * t_rows : (p + 1) * 2 * t_rows]
                + cr[p, rows, :].astype(F32)
            ).astype(BF)
            out_copy(s, p).start()
        return carry

    lax.fori_loop(0, 2, finish, 0)

    for s in range(2):
        for p in range(2):
            out_copy(s, p).wait()

    def sent(buf, sem):
        remote(buf, buf, sem, sem, row_peer(1)).wait_send()

    for kind in range(4):
        sent(xf.at[0, 0], img_s.at[kind])
    for kind in range(3):
        sent(xf.at[0, 0], sib_s.at[kind])
    for rel in (1, 2, 3):
        sent(stb.at[0], st_s.at[rel])
        sent(textb.at[0, 0], txt_s.at[rel])
    for part in range(2):
        for way in range(2):
            sent(kvb.at[0, 0:2], y_s.at[part, way])
        sent(kvb.at[0, 0:2], f_s.at[part])
    for rel, other in far_order:
        sent(osend.at[0], a_s.at[rel * 2 + other])
    for d in (1, 2, 3):
        ty(d).wait_send()
    w_first.wait_send()
    for i in range(len(zpeers)):
        w_pass(i).wait_send()


def per_device(
    nb,
    image_hidden,
    modulation,
    qkv_weight,
    out_weight,
    q_gain,
    k_gain,
    text_keys,
    text_values,
    stale_keys,
    stale_values,
    cached_residual,
    patch_of,
    refresh,
    text_len,
):
    prompts, rows, half = image_hidden.shape
    hd = q_gain.shape[0]
    channels = out_weight.shape[0]
    tw = TRI * hd
    cr_rows = rows // NC
    t_rows = rows // NT
    trow = text_keys.shape[1]
    smem = pl.BlockSpec(memory_space=pltpu.SMEM)
    vmem = pl.BlockSpec(memory_space=pltpu.VMEM)
    hbm = pl.BlockSpec(memory_space=pl.ANY)
    dma = pltpu.SemaphoreType.DMA
    ns = 2 * nb
    return pl.pallas_call(
        functools.partial(kernel, nb),
        name="joint",
        out_shape=jax.ShapeDtypeStruct(image_hidden.shape, BF),
        in_specs=[smem] * 3 + [vmem] * 4 + [hbm] * 8,
        out_specs=hbm,
        scratch_shapes=[
            pltpu.VMEM((2 * half, 3 * tw), BF),
            pltpu.VMEM((2, 4, rows, half), BF),
            pltpu.VMEM((prompts, rows, half), BF),
            pltpu.VMEM((prompts, rows, half), BF),
            pltpu.VMEM((4 * cr_rows, 2 * half), BF),
            pltpu.VMEM((4, rows, 2 * tw), BF),
            pltpu.VMEM((4, rows, 2 * tw), BF),
            pltpu.VMEM((4, rows, 3 * tw), BF),
            pltpu.VMEM((4, 4, rows, 2 * tw), BF),
            pltpu.VMEM((4, 4, trow, 2 * tw), BF),
            pltpu.VMEM((NT, TRI, 4 * t_rows, hd), F32),
            pltpu.VMEM((NT, TRI, 4 * t_rows, hd), F32),
            pltpu.VMEM((NT, TRI, 4 * t_rows, hd), F32),
            pltpu.VMEM((4, NT, t_rows, tw), BF),
            pltpu.VMEM((2, 2, 2, 2, 2 * t_rows, tw), BF),
            pltpu.VMEM((channels, half), BF),
            pltpu.VMEM((channels, half), BF),
            pltpu.VMEM((prompts, rows, half), BF),
            dma((15,)),
            dma((4,)),
            dma((NC, 4)),
            dma((3,)),
            dma((NC, 3)),
            dma((4,)),
            dma((NC, 4)),
            dma((4,)),
            dma((4,)),
            dma((3,)),
            dma((3,)),
            dma((2, 2)),
            dma((NC, 2, 2)),
            dma((2,)),
            dma((NC,)),
            dma((8,)),
            dma((2, 8)),
            dma((ns,)),
            dma((ns,)),
        ],
        compiler_params=pltpu.CompilerParams(
            collective_id=0, has_side_effects=True, vmem_limit_bytes=66 * 1024 * 1024 - 2097152
        ),
    )(
        patch_of,
        refresh,
        text_len,
        jnp.transpose(modulation, (1, 0, 2)),
        jnp.asarray(pair_frequency(hd)),
        q_gain.reshape(1, hd),
        k_gain.reshape(1, hd),
        image_hidden,
        jnp.transpose(qkv_weight, (1, 0, 2)),
        out_weight,
        text_keys,
        text_values,
        stale_keys,
        stale_values,
        cached_residual,
    )


def solution(mesh):
    in_specs = (
        P("batch", "seq", "head"),
        P("batch", None, None),
        P(None, None, "head"),
        P("head", None),
        P(),
        P(),
        P("batch", "seq", "head"),
        P("batch", "seq", "head"),
        P("batch", "seq", "head"),
        P("batch", "seq", "head"),
        P("batch", "seq", "head"),
        P("batch"),
        P("batch"),
        P("batch"),
    )
    out_specs = P("batch", "seq", "head")
    return jax.shard_map(
        functools.partial(per_device, mesh.shape["batch"]),
        mesh=mesh,
        in_specs=in_specs,
        out_specs=out_specs,
        check_vma=False,
    )
```
